32 devices in a mesh: parts: 2 (over x), shard: 16 (over z, y, core).
Axes of the slice: x: 2, y: 2, z: 4, core: 2. Of those that a mesh axis runs over, the one named last changes fastest.
Arguments:
- queries: bfloat16 [256, 32, 128], P(('parts', 'shard')), parts along dimension 0, may hold values from -6 to 6
- doc_tokens: bfloat16 [256, 128, 128], P(('parts', 'shard')), parts along dimension 0, may hold values from -0.5 to 0.5
- doc_lens: int32 [256], P(('parts', 'shard')), parts along dimension 0, may hold values from 1 to 128
- candidates: int32 [256, 128], P(('parts', 'shard')), parts along dimension 0, may hold values from 0 to 127
Outputs:
- scores: float32 [256, 128], P(('parts', 'shard')), parts along dimension 0
The draws below stay inside these ranges and needn't reach their ends.
There are 2 independent parts, one for each index of `parts`. The reference program is written for one: setup_inputs(seed, part) draws one part's arguments, and reference() takes and returns one part's arrays. A program takes and returns all parts, laid end to end along the dimension named above; each array names one. Nothing has to cross between parts.
Inputs may be any that keep to these rules, and one draw needn't show every extreme that they name: `doc_lens`: every document has at least one live row. `candidates`: ids of documents of the same part.
All inputs are finite; a program needn't handle non-finite values.
Results may differ from the reference program's by a relative error of at most 0.0003.
Values may be sent and summed in bfloat16 or wider, within the bound.
A program may use at most 64 MiB of HBM per device.

```python
import jax
import jax.numpy as jnp
from jax import lax

D = 128
QTOK = 32
BLOCK = 128
CAND = 128
QUERIES = 128
DOCS = 128


def touch_ends(result, key, low, largest):
    place = [jax.random.randint(jax.random.fold_in(key, axis), (), 0, length) for axis, length in enumerate(result.shape)]
    main_axis = result.shape.index(max(result.shape))
    next_to = place[:main_axis] + [(place[main_axis] + 1) % result.shape[main_axis]] + place[main_axis + 1:]
    return result.at[tuple(place)].set(low).at[tuple(next_to)].set(largest)


def steps_of(stream_key, dims, cuts, low, largest):
    def one(dim, blocks):
        draws = jax.random.uniform(jax.random.fold_in(jax.random.fold_in(stream_key, 6), dim), (blocks,), jnp.float32, low / len(cuts), largest / len(cuts))
        return jnp.repeat(jnp.exp(draws), dims[dim] // blocks).reshape((-1,) + (1,) * (len(dims) - dim - 1))

    factor_of = one(*cuts[0])
    for cut in cuts[1:]:
        factor_of = factor_of * one(*cut)
    return factor_of


def bell_draw(key, extent, spread, limit, pieces=(), kind=jnp.bfloat16):
    values = jax.random.normal(key, extent, jnp.float32) * spread
    if len(pieces) > 0:
        values = steps_of(key, extent, pieces, -0.22, 0.18) * values
    return jnp.clip(values, min=-limit, max=limit).astype(kind)


def setup_inputs(seed: int = 0, part: int = 0) -> dict:
    key_list = jax.random.split(jax.random.key(seed), 5)
    part_keys = jax.random.split(jax.random.fold_in(key_list[4], part), 5)
    queries = bell_draw(part_keys[0], (QUERIES, QTOK, D), 1.0, 6.0, ((0, 16),))
    doc_tokens = bell_draw(part_keys[1], (DOCS, BLOCK, D), D ** -0.5, 0.5, ((0, 16),))
    doc_lens = touch_ends(jax.random.randint(part_keys[2], (DOCS,), 1, BLOCK + 1), jax.random.fold_in(part_keys[2], 1), 1, BLOCK).astype(jnp.int32)
    candidates = touch_ends(jax.random.randint(part_keys[3], (QUERIES, CAND), 0, DOCS), jax.random.fold_in(part_keys[3], 1), 0, DOCS - 1).astype(jnp.int32)
    return dict(queries=queries, doc_tokens=doc_tokens, doc_lens=doc_lens, candidates=candidates)


def reference(queries, doc_tokens, doc_lens, candidates):
    rows = jnp.arange(doc_tokens.shape[1], dtype=jnp.int32)

    def one_query(item):
        query, picked = item
        blocks = doc_tokens[picked].astype(jnp.float32)
        live = rows[None, :] < doc_lens[picked][:, None]
        sim = jnp.einsum("id,cjd->cij", query.astype(jnp.float32), blocks)
        sim = jnp.where(live[:, None, :], sim, -1e30)
        return jnp.mean(jnp.max(sim, axis=2), axis=1)

    return lax.map(one_query, (queries, candidates))
```

```python
import functools

import jax
import jax.numpy as jnp
from jax import lax
from jax.experimental import pallas as pl
from jax.experimental.pallas import tpu as pltpu
from jax.sharding import PartitionSpec as P

LANES = 128
MESH = pl.DeviceIdType.MESH


def flip(index, mask):
    out = index
    bit = 1
    while bit <= mask:
        if mask & bit:
            out = out + bit - 2 * bit * ((index // bit) % 2)
        bit *= 2
    return out


def cut_points(docs):
    return [0, docs // 2, docs - docs // 4, docs]


def score_kernel(groups, tokens, lens_hbm, q_hbm, d_hbm, cand_hbm, out_ref,
                 lens_ref, cand_ref, qbuf, dbuf, best, outgoing, pieces,
                 local_sem, q_send, q_recv, p_send, p_recv, y_send, y_recv, f_send, f_recv, o_send, o_recv):
    part = lax.axis_index("parts")
    me = lax.axis_index("shard")
    k = lax.rem(me, 2)
    b = lax.rem(me // 2, 2)
    g = me // 4

    def at(g_, b_, k_):
        return (part, g_ * 4 + b_ * 2 + k_)

    docs, rows, width = d_hbm.shape
    q_rows = q_hbm.shape[0]
    count = q_rows // tokens
    edges = cut_points(docs)
    chunks = len(edges) - 1
    slots = {name: b_ * 2 + k_ for name, b_, k_ in
             (("me", b, k), ("partner", b, 1 - k), ("y", 1 - b, k), ("yp", 1 - b, 1 - k))}
    partner = at(g, b, 1 - k)
    across = at(g, 1 - b, k)
    corner = at(g, 1 - b, 1 - k)
    order = [1] + [j for j in range(groups - 1, 1, -1)]

    q_in = pltpu.make_async_copy(q_hbm, qbuf.at[g], local_sem.at[0])
    d_in = pltpu.make_async_copy(d_hbm, dbuf.at[slots["me"]], local_sem.at[1])
    lens_in = pltpu.make_async_copy(lens_hbm, lens_ref, local_sem.at[2])
    cand_in = pltpu.make_async_copy(cand_hbm, cand_ref, local_sem.at[3])
    lens_in.start()
    d_in.start()
    q_in.start()
    cand_in.start()

    barrier = pltpu.get_barrier_semaphore()
    takers = [at(flip(g, j), b, k) for j in order]
    for peer in takers + [partner, across, corner]:
        pl.semaphore_signal(barrier, inc=1, device_id=peer, device_id_type=MESH)

    lens_in.wait()
    d_in.wait()
    row_of = lax.broadcasted_iota(jnp.int32, (rows, width), 0)
    for j in range(docs):
        block = dbuf[slots["me"], j]
        first = jnp.broadcast_to(block[0:1, :].astype(jnp.float32), (rows, width))
        kept = jnp.where(row_of < lens_ref[j], block.astype(jnp.float32), first)
        dbuf[slots["me"], j] = kept.astype(dbuf.dtype)
    q_in.wait()
    pl.semaphore_wait(barrier, len(takers) + 3)

    def remote(src, dst, send, recv, device):
        return pltpu.make_async_remote_copy(src_ref=src, dst_ref=dst, send_sem=send, recv_sem=recv,
                                            device_id=device, device_id_type=MESH)

    def doc_chunk(name, c, send, recv, device):
        ref = dbuf.at[slots[name], pl.ds(edges[c], edges[c + 1] - edges[c])]
        return remote(ref, ref, send.at[c], recv.at[c], device)

    mine = dbuf.at[slots["me"]]
    to_partner = remote(mine, mine, p_send, p_recv, partner)
    to_across = [doc_chunk("me", c, y_send, y_recv, across) for c in range(chunks)]
    relays = [doc_chunk("y", c, f_send, f_recv, partner) for c in range(chunks - 1)]
    relays.append(doc_chunk("me", chunks - 1, f_send, f_recv, corner))
    q_out = {j: remote(qbuf.at[g], qbuf.at[g], q_send.at[j], q_recv.at[j], peer) for j, peer in zip(order, takers)}

    to_across[0].start()
    for j in order[:2]:
        q_out[j].start()
    to_partner.start()
    for j in order[2:]:
        q_out[j].start()
    for copy in to_across[1:]:
        copy.start()
    relays[-1].start()

    have = {name: 0 for name in slots}
    done = {}
    ready = []

    def dot_max(j, name, low, high):
        n = high - low
        u = flip(g, j)
        block = dbuf[slots[name], low:high].reshape(n * rows, width)
        sim = lax.dot_general(block, qbuf[u], (((1,), (1,)), ((), ())), preferred_element_type=jnp.float32)
        best[u * 4 + slots[name], low:high, :] = jnp.max(sim.reshape(n, rows, q_rows), axis=1)

    def catch_up():
        for name in slots:
            for j in ready:
                low = done.get((j, name), 0)
                if low < have[name]:
                    dot_max(j, name, low, have[name])
                    done[j, name] = have[name]

    def arrive(event):
        kind, which = event
        if kind == "q":
            q_out[which].wait_recv()
            ready.append(which)
        elif kind == "p":
            to_partner.wait_recv()
            have["partner"] = docs
        elif kind == "y":
            to_across[which].wait_recv()
            if which < chunks - 1:
                relays[which].start()
            have["y"] = edges[which + 1]
        else:
            relays[which].wait_recv()
            have["yp"] = edges[which + 1]

    ready.append(0)
    have["me"] = docs
    catch_up()
    arrive(("p", 0))
    catch_up()
    queue = [("q", j) for j in order]
    events = []
    for c in range(chunks):
        if queue:
            events.append(queue.pop(0))
        events.append(("y", c))
        if c > 0:
            events.append(("yp", c - 1))
    for event in queue:
        events.insert(len(events) - 2, event)
    events.append(("yp", chunks - 1))
    for event in events:
        arrive(event)
        catch_up()

    q_of = lax.broadcasted_iota(jnp.int32, (count, q_rows), 1) // tokens
    pick = (q_of == lax.broadcasted_iota(jnp.int32, (count, q_rows), 0)).astype(jnp.float32)
    pick = (pick * (1.0 / tokens)).astype(jnp.bfloat16)
    rest = best[...].reshape(groups * 4 * docs, q_rows)
    total = None
    for _ in range(3):
        term = rest.astype(jnp.bfloat16)
        rest = rest - term.astype(jnp.float32)
        got = lax.dot_general(pick, term, (((1,), (1,)), ((), ())), preferred_element_type=jnp.float32)
        total = got if total is None else total + got
    blocks = total.shape[1] // LANES
    for n in range(blocks):
        outgoing[n] = total[:, n * LANES:(n + 1) * LANES]

    results = [remote(outgoing, pieces.at[g], o_send.at[i], o_recv.at[i], peer) for i, peer in enumerate(takers)]
    for copy in results[::-1]:
        copy.start()
    pieces[g] = outgoing[...]
    for copy in to_across + relays + [to_partner] + list(q_out.values()):
        copy.wait_send()

    per_unit = 4 * docs
    inside = LANES // per_unit
    lane = lax.broadcasted_iota(jnp.int32, (count, LANES), 1) // per_unit
    cand_in.wait()
    cand = cand_ref[...]
    inside_of = lax.rem(cand, LANES)
    tile_of = cand // LANES
    out = None
    for copy in results:
        copy.wait_recv()
    for n in range(groups * 4 * docs // LANES):
        total = None
        for i in range(inside):
            shift = lax.rem(i - lax.rem(g, inside) + inside, inside) * per_unit
            got = pltpu.roll(pieces[n * inside + i, g // inside], shift, 1)
            total = got if total is None else jnp.where(lane == i, got, total)
        got = jnp.take_along_axis(total, inside_of, axis=1, mode="promise_in_bounds")
        out = got if out is None else jnp.where(tile_of == n, got, out)
    out_ref[...] = out
    for copy in results:
        copy.wait_send()


def body(shards, queries, doc_tokens, doc_lens, candidates):
    count, tokens, width = queries.shape
    docs, rows, _ = doc_tokens.shape
    groups = shards // 4
    chunks = len(cut_points(docs)) - 1
    q_rows = count * tokens
    blocks = groups * 4 * docs // LANES
    dma = pltpu.SemaphoreType.DMA
    return pl.pallas_call(
        functools.partial(score_kernel, groups, tokens),
        out_shape=pltpu.VMEM(candidates.shape, jnp.float32),
        in_specs=[pl.BlockSpec(memory_space=pl.ANY)] * 4,
        out_specs=pl.BlockSpec(memory_space=pltpu.VMEM),
        scratch_shapes=[
            pltpu.SMEM(doc_lens.shape, jnp.int32),
            pltpu.VMEM(candidates.shape, jnp.int32),
            pltpu.VMEM((groups, q_rows, width), queries.dtype),
            pltpu.VMEM((4, docs, rows, width), doc_tokens.dtype),
            pltpu.VMEM((groups * 4, docs, q_rows), jnp.float32),
            pltpu.VMEM((blocks, count, LANES), jnp.float32),
            pltpu.VMEM((groups, blocks, count, LANES), jnp.float32),
            dma((4,)),
            dma((groups,)), dma((groups,)),
            dma, dma,
            dma((chunks,)), dma((chunks,)),
            dma((chunks,)), dma((chunks,)),
            dma((groups,)), dma((groups,)),
        ],
        compiler_params=pltpu.CompilerParams(collective_id=0, has_side_effects=True),
    )(doc_lens, queries.reshape(q_rows, width), doc_tokens, candidates)


def solution(mesh):
    in_specs = (
        P(("parts", "shard"), None, None),
        P(("parts", "shard"), None, None),
        P(("parts", "shard")),
        P(("parts", "shard"), None),
    )
    out_specs = P(("parts", "shard"), None)
    step = functools.partial(body, mesh.shape["shard"])
    return jax.shard_map(step, mesh=mesh, in_specs=in_specs, out_specs=out_specs, check_vma=False)
```

```python
import functools

import jax
import jax.numpy as jnp
from jax import lax
from jax.experimental import pallas as pl
from jax.experimental.pallas import tpu as pltpu
from jax.sharding import PartitionSpec as P

LANES = 128
MESH = pl.DeviceIdType.MESH


def flip(index, mask):
    out = index
    bit = 1
    while bit <= mask:
        if mask & bit:
            out = out + bit - 2 * bit * ((index // bit) % 2)
        bit *= 2
    return out


def cut_points(docs):
    return [0, docs // 2, docs - docs // 4, docs]


def score_kernel(groups, tokens, lens_hbm, q_hbm, d_hbm, cand_hbm, out_ref,
                 lens_ref, cand_ref, qbuf, dbuf, best, outgoing, pieces,
                 local_sem, here, q_send, q_recv, p_send, p_recv, y_send, y_recv, f_send, f_recv, o_send, o_recv):
    part = lax.axis_index("parts")
    me = lax.axis_index("shard")
    k = lax.rem(me, 2)
    b = lax.rem(me // 2, 2)
    g = me // 4

    def at(g_, b_, k_):
        return (part, g_ * 4 + b_ * 2 + k_)

    docs, rows, width = d_hbm.shape
    q_rows = q_hbm.shape[0]
    count = q_rows // tokens
    per_unit = 4 * docs
    edges = cut_points(docs)
    chunks = len(edges) - 1
    order = list(range(1, groups))
    end = lax.rem(g + 1, 4) < 2
    mask = {j: jnp.where(end, j, j ^ 1) if j % 4 > 1 else j for j in order}
    other = {j: jnp.where(end, flip(g, j), flip(g, j ^ 1)) if j % 4 > 1 else flip(g, j) for j in order}
    other[0] = g
    partner = at(g, b, 1 - k)
    across = at(g, 1 - b, 1 - k)
    level = {j: at(other[j], b, 1 - k) for j in order}

    def remote(src, dst, send, recv, device):
        return pltpu.make_async_remote_copy(src_ref=src, dst_ref=dst, send_sem=send, recv_sem=recv,
                                            device_id=device, device_id_type=MESH)

    lens_in = pltpu.make_async_copy(lens_hbm, lens_ref, local_sem.at[0])
    q_in = pltpu.make_async_copy(q_hbm, qbuf.at[g], local_sem.at[1])
    cand_in = pltpu.make_async_copy(cand_hbm, cand_ref, local_sem.at[2])
    d_in = pltpu.make_async_copy(d_hbm, dbuf.at[0], local_sem.at[3])
    lens_in.start()
    d_in.start()
    q_in.start()
    cand_in.start()

    pairs = [(0, partner, k == 1), (1, across, b == 0)] + [(1 + mask[j], level[j], g < other[j]) for j in order]
    barrier = pltpu.get_barrier_semaphore()
    greeted = 0
    for _, peer, first in pairs:
        greeted = greeted + jnp.where(first, 0, 1)

        @pl.when(first)
        def _():
            pl.semaphore_signal(barrier, inc=1, device_id=peer, device_id_type=MESH)

    @pl.when(greeted > 0)
    def _():
        pl.semaphore_wait(barrier, greeted)

    for slot, peer, first in pairs:
        @pl.when(jnp.logical_not(first))
        def _():
            pl.semaphore_signal(here.at[slot], inc=1, device_id=peer, device_id_type=MESH)

    def meet(which):
        slot, _, first = pairs[which]

        @pl.when(first)
        def _():
            pl.semaphore_wait(here.at[slot], 1)

    mine = qbuf.at[g]
    q_out = {j: remote(mine, mine, q_send.at[mask[j]], q_recv.at[mask[j]], level[j]) for j in order}
    to_partner = remote(dbuf.at[0], dbuf.at[1], p_send, p_recv, partner)
    to_across, relays = [], []
    for c in range(chunks):
        span = pl.ds(edges[c], edges[c + 1] - edges[c])
        to_across.append(remote(dbuf.at[0, span], dbuf.at[2, span], y_send.at[c], y_recv.at[c], across))
        relays.append(remote(dbuf.at[2, span], dbuf.at[3, span], f_send.at[c], f_recv.at[c], partner))

    lens_in.wait()
    d_in.wait()
    row_of = lax.broadcasted_iota(jnp.int32, (rows, width), 0)
    for c in range(chunks):
        for j in range(edges[c], edges[c + 1]):
            block = dbuf[0, j]
            first_row = jnp.broadcast_to(block[0:1, :].astype(jnp.float32), (rows, width))
            kept = jnp.where(row_of < lens_ref[j], block.astype(jnp.float32), first_row)
            dbuf[0, j] = kept.astype(dbuf.dtype)
        if c == 0:
            meet(1)
        to_across[c].start()
    meet(0)
    to_partner.start()
    q_in.wait()

    have = [docs, 0, 0, 0]
    done = {}
    ready = []

    def dot_max(unit, which, low, high):
        block = qbuf[other[unit]]
        for j in range(low, high):
            sim = lax.dot_general(dbuf[which, j], block, (((1,), (1,)), ((), ())), preferred_element_type=jnp.float32)
            best[other[unit], which * docs + j:which * docs + j + 1, :] = jnp.max(sim, axis=0, keepdims=True)

    def catch_up():
        for which in range(4):
            for unit in ready:
                low = done.get((unit, which), 0)
                if low < have[which]:
                    dot_max(unit, which, low, have[which])
                    done[unit, which] = have[which]

    if order:
        meet(2)
        q_out[order[0]].start()
    ready.append(0)
    catch_up()
    for i, j in enumerate(order[1:]):
        meet(3 + i)
        q_out[j].start()

    cand_in.wait()
    cand = cand_ref[...]
    device = cand // docs
    same = lax.rem(device // 2, 2) == b
    source = device // 4
    holder = jnp.where(source == g, k, 1 - k)
    near = lax.rem(device, 2) == holder
    local = jnp.where(same, jnp.where(near, 0, docs), jnp.where(near, 3 * docs, 2 * docs))
    lane = lax.rem(g * per_unit, LANES) + lax.rem(cand, docs) + local

    def arrive(event):
        kind, which = event
        if kind == "p":
            to_partner.wait_recv()
            have[1] = docs
        elif kind == "q":
            q_out[which].wait_recv()
            ready.append(which)
        elif kind == "y":
            to_across[which].wait_recv()
            relays[which].start()
            have[2] = edges[which + 1]
        else:
            relays[which].wait_recv()
            have[3] = edges[which + 1]

    events = [(("p", 0), True)]
    for i in range(max(len(order), chunks)):
        if i < chunks and i:
            events += [(("r", i - 1), i == 1), (("y", i), i == 1)]
        if i < len(order):
            events.append((("q", order[i]), True))
        if i < chunks and not i:
            events.append((("y", i), True))
    events.append((("r", chunks - 1), True))
    for event, now in events:
        arrive(event)
        if now:
            catch_up()

    q_of = lax.broadcasted_iota(jnp.int32, (count, q_rows), 1) // tokens
    pick = (q_of == lax.broadcasted_iota(jnp.int32, (count, q_rows), 0)).astype(jnp.float32)
    pick = (pick * (1.0 / tokens)).astype(jnp.bfloat16)
    rest = best[...].reshape(groups * per_unit, q_rows)
    total = None
    for _ in range(2):
        term = rest.astype(jnp.bfloat16)
        rest = rest - term.astype(jnp.float32)
        got = lax.dot_general(pick, term, (((1,), (1,)), ((), ())), preferred_element_type=jnp.float32)
        total = got if total is None else total + got
    for n in range(total.shape[1] // LANES):
        outgoing[n] = total[:, n * LANES:(n + 1) * LANES]

    results = {}
    for j in order:
        results[j] = remote(outgoing.at[other[j] * per_unit // LANES], pieces.at[g], o_send.at[mask[j]],
                            o_recv.at[mask[j]], level[j])
    for copy in list(results.values())[::-1]:
        copy.start()

    def picked(piece):
        return jnp.take_along_axis(piece, lane, axis=1, mode="promise_in_bounds")

    out = picked(outgoing[g * per_unit // LANES])
    for copy in to_across + relays + [to_partner] + list(q_out.values()):
        copy.wait_send()
    for j, copy in results.items():
        copy.wait_recv()
        out = jnp.where(source == other[j], picked(pieces[other[j]]), out)
    out_ref[...] = out
    for copy in results.values():
        copy.wait_send()


def body(shards, queries, doc_tokens, doc_lens, candidates):
    count, tokens, width = queries.shape
    docs, rows, _ = doc_tokens.shape
    groups = shards // 4
    chunks = len(cut_points(docs)) - 1
    q_rows = count * tokens
    blocks = groups * 4 * docs // LANES
    dma = pltpu.SemaphoreType.DMA
    return pl.pallas_call(
        functools.partial(score_kernel, groups, tokens),
        out_shape=pltpu.VMEM(candidates.shape, jnp.float32),
        in_specs=[pl.BlockSpec(memory_space=pl.ANY)] * 4,
        out_specs=pl.BlockSpec(memory_space=pltpu.VMEM),
        scratch_shapes=[
            pltpu.SMEM(doc_lens.shape, jnp.int32),
            pltpu.VMEM(candidates.shape, jnp.int32),
            pltpu.VMEM((groups, q_rows, width), queries.dtype),
            pltpu.VMEM((4, docs, rows, width), doc_tokens.dtype),
            pltpu.VMEM((groups, 4 * docs, q_rows), jnp.float32),
            pltpu.VMEM((blocks, count, LANES), jnp.float32),
            pltpu.VMEM((groups, count, LANES), jnp.float32),
            dma((4,)),
            pltpu.SemaphoreType.REGULAR((groups + 1,)),
            dma((groups,)), dma((groups,)),
            dma, dma,
            dma((chunks,)), dma((chunks,)),
            dma((chunks,)), dma((chunks,)),
            dma((groups,)), dma((groups,)),
        ],
        compiler_params=pltpu.CompilerParams(collective_id=0, has_side_effects=True),
    )(doc_lens, queries.reshape(q_rows, width), doc_tokens, candidates)


def solution(mesh):
    in_specs = (
        P(("parts", "shard"), None, None),
        P(("parts", "shard"), None, None),
        P(("parts", "shard")),
        P(("parts", "shard"), None),
    )
    out_specs = P(("parts", "shard"), None)
    step = functools.partial(body, mesh.shape["shard"])
    return jax.shard_map(step, mesh=mesh, in_specs=in_specs, out_specs=out_specs, check_vma=False)
```

```python
import functools

import jax
import jax.numpy as jnp
from jax import lax
from jax.experimental import pallas as pl
from jax.experimental.pallas import tpu as pltpu
from jax.sharding import PartitionSpec as P

LANES = 128
MESH = pl.DeviceIdType.MESH


def flip(index, mask):
    out = index
    bit = 1
    while bit <= mask:
        if mask & bit:
            out = out + bit - 2 * bit * ((index // bit) % 2)
        bit *= 2
    return out


def cut_points(docs):
    return [0, docs // 2, docs - docs // 4, docs]


def score_kernel(groups, tokens, lens_hbm, q_hbm, d_hbm, cand_hbm, out_ref,
                 lens_ref, cand_ref, qbuf, dbuf, hbuf, best, rest_best, outgoing, pieces, extra,
                 local_sem, here, q_send, q_recv, d_send, p_recv, y_recv, f_recv, o_send, o_recv, h_send, h_recv):
    part = lax.axis_index("parts")
    me = lax.axis_index("shard")
    k = lax.rem(me, 2)
    b = lax.rem(me // 2, 2)
    g = me // 4

    def at(g_, b_, k_):
        return (part, g_ * 4 + b_ * 2 + k_)

    docs, rows, width = d_hbm.shape
    q_rows = q_hbm.shape[0]
    count = q_rows // tokens
    per_unit = 4 * docs
    edges = cut_points(docs)
    chunks = len(edges) - 1
    order = list(range(1, groups))
    end = lax.rem(g, 4) == 0
    mask = {j: jnp.where(end, j, j ^ 1) if j % 4 > 1 else j for j in order}
    other = {j: jnp.where(end, flip(g, j), flip(g, j ^ 1)) if j % 4 > 1 else flip(g, j) for j in order}
    other[0] = g
    partner = at(g, b, 1 - k)
    across = at(g, 1 - b, 1 - k)
    level = {j: at(other[j], b, 1 - k) for j in order}

    short = groups % 4 == 0
    late = edges[-2]
    tail = docs - late
    home = jnp.logical_and(lax.rem(g, 4) == 0, b == 0)
    sooner = jnp.logical_and(lax.rem(g, 4) == 3, b == 0)
    giver = jnp.logical_and(lax.rem(g, 4) == 3, b == 1)
    top = flip(g, 3)

    def remote(src, dst, send, recv, device):
        return pltpu.make_async_remote_copy(src_ref=src, dst_ref=dst, send_sem=send, recv_sem=recv,
                                            device_id=device, device_id_type=MESH)

    lens_in = pltpu.make_async_copy(lens_hbm, lens_ref, local_sem.at[0])
    q_in = pltpu.make_async_copy(q_hbm, qbuf.at[g], local_sem.at[1])
    cand_in = pltpu.make_async_copy(cand_hbm, cand_ref, local_sem.at[2])
    d_in = pltpu.make_async_copy(d_hbm, dbuf.at[0], local_sem.at[3])
    lens_in.start()
    d_in.start()
    q_in.start()
    cand_in.start()

    pairs = [(0, partner, k == 1), (1, across, b == 0)] + [(1 + mask[j], level[j], g < other[j]) for j in order]
    barrier = pltpu.get_barrier_semaphore()
    greeted = 0
    for _, peer, first in pairs:
        greeted = greeted + jnp.where(first, 0, 1)

        @pl.when(first)
        def _():
            pl.semaphore_signal(barrier, inc=1, device_id=peer, device_id_type=MESH)

    if short:
        greeted = greeted + jnp.where(giver, 1, 0)

        @pl.when(home)
        def _():
            pl.semaphore_signal(barrier, inc=1, device_id=at(top, 1, 1 - k), device_id_type=MESH)

    @pl.when(greeted > 0)
    def _():
        pl.semaphore_wait(barrier, greeted)

    for slot, peer, first in pairs:
        @pl.when(jnp.logical_not(first))
        def _():
            pl.semaphore_signal(here.at[slot], inc=1, device_id=peer, device_id_type=MESH)

    def meet(which):
        slot, _, first = pairs[which]

        @pl.when(first)
        def _():
            pl.semaphore_wait(here.at[slot], 1)

    mine = qbuf.at[g]
    q_out = {j: remote(mine, mine, q_send, q_recv.at[mask[j] - 1], level[j]) for j in order}
    to_partner = remote(dbuf.at[0], dbuf.at[1], d_send, p_recv, partner)
    to_across, relays = [], []
    for c in range(chunks):
        span = pl.ds(edges[c], edges[c + 1] - edges[c])
        to_across.append(remote(dbuf.at[0, span], dbuf.at[2, span], d_send, y_recv.at[c], across))
        relays.append(remote(dbuf.at[2, span], dbuf.at[3, span], d_send, f_recv.at[c], partner))

    lens_in.wait()
    d_in.wait()
    row_of = lax.broadcasted_iota(jnp.int32, (rows, width), 0)
    for c in range(chunks):
        for j in range(edges[c], edges[c + 1]):
            block = dbuf[0, j]
            first_row = jnp.broadcast_to(block[0:1, :].astype(jnp.float32), (rows, width))
            kept = jnp.where(row_of < lens_ref[j], block.astype(jnp.float32), first_row)
            dbuf[0, j] = kept.astype(dbuf.dtype)
        if c == 0:
            meet(1)
        to_across[c].start()
    meet(0)
    to_partner.start()
    q_in.wait()

    def dot_max(unit, which, low, high):
        block = qbuf[other[unit]]
        for j in range(low, high):
            sim = lax.dot_general(dbuf[which, j], block, (((1,), (1,)), ((), ())), preferred_element_type=jnp.float32)
            best[other[unit], which * docs + j:which * docs + j + 1, :] = jnp.max(sim, axis=0, keepdims=True)

    def catch_up(have, ready, done):
        for which in range(4):
            for unit in ready:
                low = done.get((unit, which), 0)
                if low < have[which]:
                    dot_max(unit, which, low, have[which])
                    done[unit, which] = have[which]

    if order:
        meet(2)
        q_out[order[0]].start()
    dot_max(0, 0, 0, docs)
    for i, j in enumerate(order[1:]):
        meet(3 + i)
        q_out[j].start()

    give = remote(dbuf.at[0, pl.ds(late, tail)], hbuf.at[0], h_send, h_recv.at[0], at(top, 0, 1 - k))
    share = remote(hbuf.at[0], hbuf.at[1], h_send, h_recv.at[1], partner)
    cand_in.wait()
    cand = cand_ref[...]
    device = cand // docs
    same = lax.rem(device // 2, 2) == b
    source = device // 4
    holder = jnp.where(source == g, k, 1 - k)
    near = lax.rem(device, 2) == holder
    local = jnp.where(same, jnp.where(near, 0, docs), jnp.where(near, 3 * docs, 2 * docs))
    lane = lax.rem(cand, docs) + local

    q_of = lax.broadcasted_iota(jnp.int32, (count, q_rows), 1) // tokens
    pick = (q_of == lax.broadcasted_iota(jnp.int32, (count, q_rows), 0)).astype(jnp.float32)
    pick = (pick * (1.0 / tokens)).astype(jnp.bfloat16)

    def means(rest):
        total = None
        for _ in range(2):
            term = rest.astype(jnp.bfloat16)
            rest = rest - term.astype(jnp.float32)
            got = lax.dot_general(pick, term, (((1,), (1,)), ((), ())), preferred_element_type=jnp.float32)
            total = got if total is None else total + got
        return total

    def widened(few):
        return jnp.concatenate([few, jnp.zeros((count, LANES - few.shape[1]), jnp.float32)], axis=1)

    results = {j: remote(outgoing.at[j], pieces.at[g], o_send, o_recv, level[j]) for j in order}

    def run(plan):
        have, ready, done = [docs, 0, 0, 0], [0], {(0, 0): docs}
        for kind, which, now in plan:
            if kind == "p":
                to_partner.wait_recv()
                have[1] = docs
            elif kind == "q":
                q_out[which].wait_recv()
                ready.append(which)
            elif kind == "y":
                to_across[which].wait_recv()
                relays[which].start()
                have[2] = edges[which + 1]
            elif kind == "r":
                relays[which].wait_recv()
                have[3] = edges[which + 1]
            elif kind == "give":
                @pl.when(giver)
                def _():
                    give.start()
            else:
                def answer():
                    outgoing[which] = widened(means(best[other[which]]))
                    if which:
                        results[which].start()

                if kind == "soon":
                    pl.when(sooner)(answer)
                elif short and which == 2 and now:
                    pl.when(jnp.logical_not(sooner))(answer)
                else:
                    answer()
                continue
            if now:
                catch_up(have, ready, done)

    docs_first = [("p", 0, True)] + [("q", j, True) for j in order[:1]]
    for c in range(chunks):
        docs_first += [("y", c, True)] + [("r", c - 1, True)] * (c > 0)
    docs_first.append(("r", chunks - 1, True))
    docs_first += [("s", j, False) for j in order[:1]]
    for j in order[1:]:
        docs_first += [("q", j, True), ("s", j, False)]
    docs_first.append(("s", 0, False))
    docs_last = [("p", 0, True)]
    for i in range(max(len(order), chunks)):
        if i < chunks and i:
            docs_last += [("r", i - 1, True)]
            if short and i == chunks - 1:
                docs_last += [("soon", 2, True)]
            docs_last += [("y", i, i == 1)]
        if i < len(order):
            docs_last.append(("q", order[i], True))
        if i < chunks and not i:
            docs_last += [("y", i, True)] + [("give", 0, False)] * short
    docs_last.append(("r", chunks - 1, True))
    docs_last += [("s", j, True) for j in order[::-1] + [0]]
    low = lax.rem(g, 4) < 2

    @pl.when(low)
    def _():
        run(docs_first)

    @pl.when(jnp.logical_not(low))
    def _():
        run(docs_last)

    if short:
        @pl.when(home)
        def _():
            give.wait_recv()
            share.start()
            for n in range(2):
                if n:
                    share.wait_recv()
                for j in range(tail):
                    sim = lax.dot_general(hbuf[n, j], qbuf[g], (((1,), (1,)), ((), ())), preferred_element_type=jnp.float32)
                    rest_best[n * tail + j:n * tail + j + 1, :] = jnp.max(sim, axis=0, keepdims=True)
            extra[...] = widened(means(rest_best[...]))

        @pl.when(jnp.logical_or(home, giver))
        def _():
            give.wait_send()

    def picked(piece, lanes):
        return jnp.take_along_axis(piece, lanes, axis=1, mode="promise_in_bounds")

    sent = [remote(dbuf.at[pl.ds(0, 3)], dbuf.at[pl.ds(0, 3)], d_send, p_recv, partner)]
    if order:
        sent.append(remote(qbuf.at[pl.ds(0, groups - 1)], qbuf.at[pl.ds(0, groups - 1)], q_send, p_recv, partner))
    out = picked(outgoing[0], lane)
    for copy in sent:
        copy.wait_send()
    if order:
        back = remote(pieces.at[pl.ds(0, groups - 1)], pieces.at[pl.ds(0, groups - 1)], o_send, o_recv, partner)
        back.wait_recv()
        for j in order:
            out = jnp.where(source == other[j], picked(pieces[other[j]], lane), out)
        back.wait_send()
    if short:
        row = lax.rem(cand, docs) - late
        whole = (source == top) & jnp.logical_not(same) & (row >= 0) & home
        out = jnp.where(whole, picked(extra[...], jnp.where(whole, row + jnp.where(near, 0, tail), 0)), out)
    out_ref[...] = out


def body(shards, queries, doc_tokens, doc_lens, candidates):
    count, tokens, width = queries.shape
    docs, rows, _ = doc_tokens.shape
    groups = shards // 4
    chunks = len(cut_points(docs)) - 1
    tail = docs - cut_points(docs)[-2]
    q_rows = count * tokens
    dma = pltpu.SemaphoreType.DMA
    return pl.pallas_call(
        functools.partial(score_kernel, groups, tokens),
        out_shape=pltpu.VMEM(candidates.shape, jnp.float32),
        in_specs=[pl.BlockSpec(memory_space=pl.ANY)] * 4,
        out_specs=pl.BlockSpec(memory_space=pltpu.VMEM),
        scratch_shapes=[
            pltpu.SMEM(doc_lens.shape, jnp.int32),
            pltpu.VMEM(candidates.shape, jnp.int32),
            pltpu.VMEM((groups, q_rows, width), queries.dtype),
            pltpu.VMEM((4, docs, rows, width), doc_tokens.dtype),
            pltpu.VMEM((2, tail, rows, width), doc_tokens.dtype),
            pltpu.VMEM((groups, 4 * docs, q_rows), jnp.float32),
            pltpu.VMEM((2 * tail, q_rows), jnp.float32),
            pltpu.VMEM((groups, count, LANES), jnp.float32),
            pltpu.VMEM((groups, count, LANES), jnp.float32),
            pltpu.VMEM((count, LANES), jnp.float32),
            dma((4,)),
            pltpu.SemaphoreType.REGULAR((groups + 1,)),
            dma, dma((groups - 1,)),
            dma, dma, dma((chunks,)), dma((chunks,)),
            dma, dma,
            dma, dma((2,)),
        ],
        compiler_params=pltpu.CompilerParams(collective_id=0, has_side_effects=True),
    )(doc_lens, queries.reshape(q_rows, width), doc_tokens, candidates)


def solution(mesh):
    in_specs = (
        P(("parts", "shard"), None, None),
        P(("parts", "shard"), None, None),
        P(("parts", "shard")),
        P(("parts", "shard"), None),
    )
    out_specs = P(("parts", "shard"), None)
    step = functools.partial(body, mesh.shape["shard"])
    return jax.shard_map(step, mesh=mesh, in_specs=in_specs, out_specs=out_specs, check_vma=False)
```

```python
import functools

import jax
import jax.numpy as jnp
from jax import lax
from jax.experimental import pallas as pl
from jax.experimental.pallas import tpu as pltpu
from jax.sharding import PartitionSpec as P

LANES = 128
MESH = pl.DeviceIdType.MESH


def flip(index, mask):
    out = index
    bit = 1
    while bit <= mask:
        if mask & bit:
            out = out + bit - 2 * bit * ((index // bit) % 2)
        bit *= 2
    return out


def cut_points(docs):
    return [0, docs // 2, docs - docs // 4, docs]


def score_kernel(groups, tokens, lens_hbm, q_hbm, d_hbm, cand_hbm, out_ref,
                 lens_ref, cand_ref, qbuf, dbuf, hbuf, best, rest_best, outgoing, whole, pieces, extra,
                 local_sem, here, q_send, q_recv, d_send, p_recv, y_recv, f_recv, o_send, o_recv, h_send, h_recv):
    part = lax.axis_index("parts")
    me = lax.axis_index("shard")
    k = lax.rem(me, 2)
    b = lax.rem(me // 2, 2)
    g = me // 4

    def at(g_, b_, k_):
        return (part, g_ * 4 + b_ * 2 + k_)

    docs, rows, width = d_hbm.shape
    q_rows = q_hbm.shape[0]
    count = q_rows // tokens
    per_unit = 4 * docs
    edges = cut_points(docs)
    chunks = len(edges) - 1
    order = list(range(1, groups))
    end = lax.rem(g, 4) == 0
    mask = {j: jnp.where(end, j, j ^ 1) if j % 4 > 1 else j for j in order}
    other = {j: jnp.where(end, flip(g, j), flip(g, j ^ 1)) if j % 4 > 1 else flip(g, j) for j in order}
    other[0] = g
    partner = at(g, b, 1 - k)
    across = at(g, 1 - b, 1 - k)
    level = {j: at(other[j], b, 1 - k) for j in order}

    short = groups % 4 == 0
    late = edges[-2]
    tail = docs - late
    home = jnp.logical_and(lax.rem(g, 4) == 0, b == 0)
    sooner = jnp.logical_and(lax.rem(g, 4) == 3, b == 0)
    giver = jnp.logical_and(lax.rem(g, 4) == 3, b == 1)
    top = flip(g, 3)

    def remote(src, dst, send, recv, device):
        return pltpu.make_async_remote_copy(src_ref=src, dst_ref=dst, send_sem=send, recv_sem=recv,
                                            device_id=device, device_id_type=MESH)

    lens_in = pltpu.make_async_copy(lens_hbm, lens_ref, local_sem.at[0])
    q_in = pltpu.make_async_copy(q_hbm, qbuf.at[g], local_sem.at[1])
    cand_in = pltpu.make_async_copy(cand_hbm, cand_ref, local_sem.at[2])
    d_in = pltpu.make_async_copy(d_hbm, dbuf.at[0], local_sem.at[3])
    lens_in.start()
    d_in.start()
    q_in.start()
    cand_in.start()

    pairs = [(0, partner, k == 1), (1, across, b == 0)] + [(1 + mask[j], level[j], g < other[j]) for j in order]
    barrier = pltpu.get_barrier_semaphore()
    greeted = 0
    for _, peer, first in pairs:
        greeted = greeted + jnp.where(first, 0, 1)

        @pl.when(first)
        def _():
            pl.semaphore_signal(barrier, inc=1, device_id=peer, device_id_type=MESH)

    if short:
        greeted = greeted + jnp.where(giver, 1, 0)

        @pl.when(home)
        def _():
            pl.semaphore_signal(barrier, inc=1, device_id=at(top, 1, 1 - k), device_id_type=MESH)

    @pl.when(greeted > 0)
    def _():
        pl.semaphore_wait(barrier, greeted)

    for slot, peer, first in pairs:
        @pl.when(jnp.logical_not(first))
        def _():
            pl.semaphore_signal(here.at[slot], inc=1, device_id=peer, device_id_type=MESH)

    def meet(which):
        slot, _, first = pairs[which]

        @pl.when(first)
        def _():
            pl.semaphore_wait(here.at[slot], 1)

    mine = qbuf.at[g]
    q_out = {j: remote(mine, mine, q_send, q_recv.at[mask[j] - 1], level[j]) for j in order}
    to_partner = remote(dbuf.at[0], dbuf.at[1], d_send, p_recv, partner)
    to_across, relays = [], []
    for c in range(chunks):
        span = pl.ds(edges[c], edges[c + 1] - edges[c])
        to_across.append(remote(dbuf.at[0, span], dbuf.at[2, span], d_send, y_recv.at[c], across))
        relays.append(remote(dbuf.at[2, span], dbuf.at[3, span], d_send, f_recv.at[c], partner))

    lens_in.wait()
    d_in.wait()
    row_of = lax.broadcasted_iota(jnp.int32, (rows, width), 0)
    for c in range(chunks):
        for j in range(edges[c], edges[c + 1]):
            block = dbuf[0, j]
            first_row = jnp.broadcast_to(block[0:1, :].astype(jnp.float32), (rows, width))
            kept = jnp.where(row_of < lens_ref[j], block.astype(jnp.float32), first_row)
            dbuf[0, j] = kept.astype(dbuf.dtype)
        if c == 0:
            meet(1)
        to_across[c].start()
    meet(0)
    to_partner.start()
    q_in.wait()

    def dot_max(unit, which, low, high):
        block = qbuf[other[unit]]
        for j in range(low, high):
            sim = lax.dot_general(dbuf[which, j], block, (((1,), (1,)), ((), ())), preferred_element_type=jnp.float32)
            best[other[unit], which * docs + j:which * docs + j + 1, :] = jnp.max(sim, axis=0, keepdims=True)

    def catch_up(have, units, done):
        for which in range(4):
            for unit in units:
                low = done.get((unit, which), 0)
                if low < have[which]:
                    dot_max(unit, which, low, have[which])
                    done[unit, which] = have[which]

    if order:
        meet(2)
        q_out[order[0]].start()
    dot_max(0, 0, 0, docs)
    for i, j in enumerate(order[1:]):
        meet(3 + i)
        q_out[j].start()

    give = remote(dbuf.at[0, pl.ds(late, tail)], hbuf.at[0], h_send, h_recv.at[0], at(top, 0, 1 - k))
    share = remote(hbuf.at[0], hbuf.at[1], h_send, h_recv.at[1], partner)
    cand_in.wait()
    cand = cand_ref[...]
    device = cand // docs
    same = lax.rem(device // 2, 2) == b
    source = device // 4
    holder = jnp.where(source == g, k, 1 - k)
    near = lax.rem(device, 2) == holder
    local = jnp.where(same, jnp.where(near, 0, docs), jnp.where(near, 3 * docs, 2 * docs))
    lane = lax.rem(g * per_unit, LANES) + lax.rem(cand, docs) + local

    q_of = lax.broadcasted_iota(jnp.int32, (count, q_rows), 1) // tokens
    pick = (q_of == lax.broadcasted_iota(jnp.int32, (count, q_rows), 0)).astype(jnp.float32)
    pick = (pick * (1.0 / tokens)).astype(jnp.bfloat16)

    def means(rest):
        total = None
        for _ in range(2):
            term = rest.astype(jnp.bfloat16)
            rest = rest - term.astype(jnp.float32)
            got = lax.dot_general(pick, term, (((1,), (1,)), ((), ())), preferred_element_type=jnp.float32)
            total = got if total is None else total + got
        return total

    def widened(few):
        return jnp.concatenate([few, jnp.zeros((count, LANES - few.shape[1]), jnp.float32)], axis=1)

    blocks = groups * per_unit // LANES
    results = {j: remote(outgoing.at[j], pieces.at[g], o_send, o_recv, level[j]) for j in order}
    at_once = {j: remote(whole.at[other[j] * per_unit // LANES], pieces.at[g], o_send, o_recv, level[j]) for j in order}

    def run(plan):
        have, ready, done = [docs, 0, 0, 0], [0], {(0, 0): docs}
        for kind, which, now in plan:
            if kind == "p":
                to_partner.wait_recv()
                have[1] = docs
            elif kind == "q":
                q_out[which].wait_recv()
                ready.append(which)
            elif kind == "y":
                to_across[which].wait_recv()
                relays[which].start()
                have[2] = edges[which + 1]
            elif kind == "r":
                relays[which].wait_recv()
                have[3] = edges[which + 1]
            elif kind == "give":
                @pl.when(giver)
                def _():
                    give.start()
            elif kind == "share":
                @pl.when(home)
                def _():
                    give.wait_recv()
                    share.start()
            elif kind == "rest":
                catch_up(have, ready, done)
                total = means(best[...].reshape(groups * per_unit, q_rows))
                for n in range(blocks):
                    whole[n] = total[:, n * LANES:(n + 1) * LANES]
                for j in order[::-1]:
                    if j != which:
                        at_once[j].start()
                outgoing[0] = whole[g * per_unit // LANES]
            elif kind in ("answer", "soon"):
                def answer():
                    few = widened(means(best[other[which]]))
                    if kind == "answer":
                        few = pltpu.roll(few, lax.rem(other[which] * per_unit, LANES), 1)
                    outgoing[which] = few
                    if which:
                        results[which].start()

                if now is True:
                    answer()
                else:
                    pl.when(now)(answer)
                continue
            if now:
                catch_up(have, ready if now is True else now, done)

    last = chunks - 1
    docs_first = [("p", 0, True)] + [("q", j, True) for j in order[:1]]
    for c in range(chunks):
        docs_first += [("y", c, True)] + [("r", c - 1, True)] * (c > 0)
    docs_first.append(("r", last, True))
    docs_first += [("answer", j, True) for j in order[:1]]
    for j in order[1:]:
        docs_first += [("q", j, True), ("answer", j, True)] + [("share", 0, False)] * (short and j == 2)
    docs_first.append(("answer", 0, True))

    def opening(hand):
        return ([("p", 0, True)] + [("q", j, True) for j in order[:1]] + [("give", 0, False)] * hand
                + [("y", 0, True)] + [step for c in range(1, last) for step in (("y", c, False), ("r", c - 1, True))]
                + [("q", j, True) for j in order[1:2]] + [("y", last, False)])

    far = [("q", j, True) for j in order[2:]]
    if short:
        third = opening(False) + far + [("r", last - 1, False), ("r", last, (3,)), ("soon", 3, True), ("rest", 3, False)]
        fourth = opening(True) + [("r", last - 1, (2,)), ("soon", 2, sooner)] + far
        fourth += [("r", last, (2,)), ("soon", 2, jnp.logical_not(sooner)), ("rest", 2, False)]
        plans = [(lax.rem(g, 4) < 2, docs_first), (lax.rem(g, 4) == 2, third), (lax.rem(g, 4) == 3, fourth)]
    else:
        plans = [(True, docs_first)]
    for when, plan in plans:
        if when is True:
            run(plan)
        else:
            pl.when(when)(functools.partial(run, plan))

    if short:
        @pl.when(home)
        def _():
            share.wait_recv()
            for n in range(2):
                for j in range(tail):
                    sim = lax.dot_general(hbuf[n, j], qbuf[g], (((1,), (1,)), ((), ())), preferred_element_type=jnp.float32)
                    rest_best[n * tail + j:n * tail + j + 1, :] = jnp.max(sim, axis=0, keepdims=True)
            extra[...] = widened(means(rest_best[...]))

        @pl.when(jnp.logical_or(home, giver))
        def _():
            give.wait_send()

    def picked(piece, lanes):
        return jnp.take_along_axis(piece, lanes, axis=1, mode="promise_in_bounds")

    sent = [remote(dbuf.at[pl.ds(0, 3)], dbuf.at[pl.ds(0, 3)], d_send, p_recv, partner)]
    if order:
        sent.append(remote(qbuf.at[pl.ds(0, groups - 1)], qbuf.at[pl.ds(0, groups - 1)], q_send, p_recv, partner))
    out = picked(outgoing[0], lane)
    for copy in sent:
        copy.wait_send()
    if order:
        back = remote(pieces.at[pl.ds(0, groups - 1)], pieces.at[pl.ds(0, groups - 1)], o_send, o_recv, partner)
        back.wait_recv()
        for j in order:
            out = jnp.where(source == other[j], picked(pieces[other[j]], lane), out)
        back.wait_send()
    if short:
        row = lax.rem(cand, docs) - late
        mine_whole = (source == top) & jnp.logical_not(same) & (row >= 0) & home
        out = jnp.where(mine_whole, picked(extra[...], jnp.where(mine_whole, row + jnp.where(near, 0, tail), 0)), out)
    out_ref[...] = out


def body(shards, queries, doc_tokens, doc_lens, candidates):
    count, tokens, width = queries.shape
    docs, rows, _ = doc_tokens.shape
    groups = shards // 4
    chunks = len(cut_points(docs)) - 1
    tail = docs - cut_points(docs)[-2]
    q_rows = count * tokens
    blocks = groups * 4 * docs // LANES
    dma = pltpu.SemaphoreType.DMA
    return pl.pallas_call(
        functools.partial(score_kernel, groups, tokens),
        out_shape=pltpu.VMEM(candidates.shape, jnp.float32),
        in_specs=[pl.BlockSpec(memory_space=pl.ANY)] * 4,
        out_specs=pl.BlockSpec(memory_space=pltpu.VMEM),
        scratch_shapes=[
            pltpu.SMEM(doc_lens.shape, jnp.int32),
            pltpu.VMEM(candidates.shape, jnp.int32),
            pltpu.VMEM((groups, q_rows, width), queries.dtype),
            pltpu.VMEM((4, docs, rows, width), doc_tokens.dtype),
            pltpu.VMEM((2, tail, rows, width), doc_tokens.dtype),
            pltpu.VMEM((groups, 4 * docs, q_rows), jnp.float32),
            pltpu.VMEM((2 * tail, q_rows), jnp.float32),
            pltpu.VMEM((groups, count, LANES), jnp.float32),
            pltpu.VMEM((blocks, count, LANES), jnp.float32),
            pltpu.VMEM((groups, count, LANES), jnp.float32),
            pltpu.VMEM((count, LANES), jnp.float32),
            dma((4,)),
            pltpu.SemaphoreType.REGULAR((groups + 1,)),
            dma, dma((groups - 1,)),
            dma, dma, dma((chunks,)), dma((chunks,)),
            dma, dma,
            dma, dma((2,)),
        ],
        compiler_params=pltpu.CompilerParams(collective_id=0, has_side_effects=True),
    )(doc_lens, queries.reshape(q_rows, width), doc_tokens, candidates)


def solution(mesh):
    in_specs = (
        P(("parts", "shard"), None, None),
        P(("parts", "shard"), None, None),
        P(("parts", "shard")),
        P(("parts", "shard"), None),
    )
    out_specs = P(("parts", "shard"), None)
    step = functools.partial(body, mesh.shape["shard"])
    return jax.shard_map(step, mesh=mesh, in_specs=in_specs, out_specs=out_specs, check_vma=False)
```

```python
import functools

import jax
import jax.numpy as jnp
from jax import lax
from jax.experimental import pallas as pl
from jax.experimental.pallas import tpu as pltpu
from jax.sharding import PartitionSpec as P

LANES = 128
MESH = pl.DeviceIdType.MESH


def flip(index, mask):
    out = index
    bit = 1
    while bit <= mask:
        if mask & bit:
            out = out + bit - 2 * bit * ((index // bit) % 2)
        bit *= 2
    return out


def cut_points(docs):
    return [0, 3, 5, 8]


def score_kernel(groups, tokens, lens_hbm, q_hbm, d_hbm, cand_hbm, out_ref,
                 lens_ref, cand_ref, qbuf, dbuf, hbuf, best, rest_best, outgoing, whole, pieces, extra,
                 local_sem, here, q_send, q_recv, d_send, p_recv, y_recv, f_recv, o_send, o_recv, h_send, h_recv):
    part = lax.axis_index("parts")
    me = lax.axis_index("shard")
    k = lax.rem(me, 2)
    b = lax.rem(me // 2, 2)
    g = me // 4

    def at(g_, b_, k_):
        return (part, g_ * 4 + b_ * 2 + k_)

    docs, rows, width = d_hbm.shape
    q_rows = q_hbm.shape[0]
    count = q_rows // tokens
    per_unit = 4 * docs
    edges = cut_points(docs)
    chunks = len(edges) - 1
    order = list(range(1, groups))
    end = lax.rem(g, 4) == 0
    mask = {j: jnp.where(end, j, j ^ 1) if j % 4 > 1 else j for j in order}
    other = {j: jnp.where(end, flip(g, j), flip(g, j ^ 1)) if j % 4 > 1 else flip(g, j) for j in order}
    other[0] = g
    partner = at(g, b, 1 - k)
    across = at(g, 1 - b, 1 - k)
    level = {j: at(other[j], b, 1 - k) for j in order}

    short = groups % 4 == 0
    late = edges[-2]
    tail = docs - late
    home = jnp.logical_and(lax.rem(g, 4) == 0, b == 0)
    sooner = jnp.logical_and(lax.rem(g, 4) == 3, b == 0)
    giver = jnp.logical_and(lax.rem(g, 4) == 3, b == 1)
    top = flip(g, 3)

    def remote(src, dst, send, recv, device):
        return pltpu.make_async_remote_copy(src_ref=src, dst_ref=dst, send_sem=send, recv_sem=recv,
                                            device_id=device, device_id_type=MESH)

    lens_in = pltpu.make_async_copy(lens_hbm, lens_ref, local_sem.at[0])
    q_in = pltpu.make_async_copy(q_hbm, qbuf.at[g], local_sem.at[1])
    cand_in = pltpu.make_async_copy(cand_hbm, cand_ref, local_sem.at[2])
    d_in = pltpu.make_async_copy(d_hbm, dbuf.at[0], local_sem.at[3])
    lens_in.start()
    d_in.start()
    q_in.start()
    cand_in.start()

    pairs = [(0, partner, k == 1), (1, across, b == 0)] + [(1 + mask[j], level[j], g < other[j]) for j in order]
    barrier = pltpu.get_barrier_semaphore()
    greeted = 0
    for _, peer, first in pairs:
        greeted = greeted + jnp.where(first, 0, 1)

        @pl.when(first)
        def _():
            pl.semaphore_signal(barrier, inc=1, device_id=peer, device_id_type=MESH)

    if short:
        greeted = greeted + jnp.where(giver, 1, 0)

        @pl.when(home)
        def _():
            pl.semaphore_signal(barrier, inc=1, device_id=at(top, 1, 1 - k), device_id_type=MESH)

    @pl.when(greeted > 0)
    def _():
        pl.semaphore_wait(barrier, greeted)

    for slot, peer, first in pairs:
        @pl.when(jnp.logical_not(first))
        def _():
            pl.semaphore_signal(here.at[slot], inc=1, device_id=peer, device_id_type=MESH)

    def meet(which):
        slot, _, first = pairs[which]

        @pl.when(first)
        def _():
            pl.semaphore_wait(here.at[slot], 1)

    mine = qbuf.at[g]
    q_out = {j: remote(mine, mine, q_send, q_recv.at[mask[j] - 1], level[j]) for j in order}
    to_partner = remote(dbuf.at[0], dbuf.at[1], d_send, p_recv, partner)
    to_across, relays = [], []
    for c in range(chunks):
        span = pl.ds(edges[c], edges[c + 1] - edges[c])
        to_across.append(remote(dbuf.at[0, span], dbuf.at[2, span], d_send, y_recv.at[c], across))
        relays.append(remote(dbuf.at[2, span], dbuf.at[3, span], d_send, f_recv.at[c], partner))

    lens_in.wait()
    d_in.wait()
    row_of = lax.broadcasted_iota(jnp.int32, (rows, width), 0)
    for c in range(chunks):
        for j in range(edges[c], edges[c + 1]):
            block = dbuf[0, j]
            first_row = jnp.broadcast_to(block[0:1, :].astype(jnp.float32), (rows, width))
            kept = jnp.where(row_of < lens_ref[j], block.astype(jnp.float32), first_row)
            dbuf[0, j] = kept.astype(dbuf.dtype)
        if c == 0:
            meet(1)
        to_across[c].start()
    meet(0)
    to_partner.start()
    q_in.wait()

    def dot_max(unit, which, low, high):
        block = qbuf[other[unit]]
        for j in range(low, high):
            sim = lax.dot_general(dbuf[which, j], block, (((1,), (1,)), ((), ())), preferred_element_type=jnp.float32)
            best[other[unit], which * docs + j:which * docs + j + 1, :] = jnp.max(sim, axis=0, keepdims=True)

    def catch_up(have, units, done):
        for which in range(4):
            for unit in units:
                low = done.get((unit, which), 0)
                if low < have[which]:
                    dot_max(unit, which, low, have[which])
                    done[unit, which] = have[which]

    if order:
        meet(2)
        q_out[order[0]].start()
    dot_max(0, 0, 0, docs)
    swapped = lax.rem(g, 4) == 2
    for j in order[1:]:
        out_mask, out_level = mask[j], other[j]
        if short and j % 4 > 1:
            out_mask = jnp.where(swapped, mask[j ^ 1], out_mask)
            out_level = jnp.where(swapped, other[j ^ 1], out_level)

        @pl.when(g < out_level)
        def _():
            pl.semaphore_wait(here.at[1 + out_mask], 1)

        remote(mine, mine, q_send, q_recv.at[out_mask - 1], at(out_level, b, 1 - k)).start()

    give = remote(dbuf.at[0, pl.ds(late, tail)], hbuf.at[0], h_send, h_recv.at[0], at(top, 0, 1 - k))
    share = remote(hbuf.at[0], hbuf.at[1], h_send, h_recv.at[1], partner)
    cand_in.wait()
    cand = cand_ref[...]
    device = cand // docs
    same = lax.rem(device // 2, 2) == b
    source = device // 4
    holder = jnp.where(source == g, k, 1 - k)
    near = lax.rem(device, 2) == holder
    local = jnp.where(same, jnp.where(near, 0, docs), jnp.where(near, 3 * docs, 2 * docs))
    lane = lax.rem(g * per_unit, LANES) + lax.rem(cand, docs) + local

    q_of = lax.broadcasted_iota(jnp.int32, (count, q_rows), 1) // tokens
    pick = (q_of == lax.broadcasted_iota(jnp.int32, (count, q_rows), 0)).astype(jnp.float32)
    pick = (pick * (1.0 / tokens)).astype(jnp.bfloat16)

    def means(rest):
        total = None
        for _ in range(2):
            term = rest.astype(jnp.bfloat16)
            rest = rest - term.astype(jnp.float32)
            got = lax.dot_general(pick, term, (((1,), (1,)), ((), ())), preferred_element_type=jnp.float32)
            total = got if total is None else total + got
        return total

    def widened(few):
        return jnp.concatenate([few, jnp.zeros((count, LANES - few.shape[1]), jnp.float32)], axis=1)

    blocks = groups * per_unit // LANES
    results = {j: remote(outgoing.at[j], pieces.at[g], o_send, o_recv, level[j]) for j in order}
    at_once = {j: remote(whole.at[other[j] * per_unit // LANES], pieces.at[g], o_send, o_recv, level[j]) for j in order}

    def run(plan):
        have, ready, done = [docs, 0, 0, 0], [0], {(0, 0): docs}
        for kind, which, now in plan:
            if kind == "p":
                to_partner.wait_recv()
                have[1] = docs
            elif kind == "q":
                q_out[which].wait_recv()
                ready.append(which)
            elif kind == "y":
                to_across[which].wait_recv()
                relays[which].start()
                have[2] = edges[which + 1]
            elif kind == "r":
                relays[which].wait_recv()
                have[3] = edges[which + 1]
            elif kind == "give":
                @pl.when(giver)
                def _():
                    give.start()
            elif kind == "share":
                @pl.when(home)
                def _():
                    give.wait_recv()
                    share.start()
            elif kind == "rest":
                catch_up(have, ready, done)
                total = means(best[...].reshape(groups * per_unit, q_rows))
                for n in range(blocks):
                    whole[n] = total[:, n * LANES:(n + 1) * LANES]
                for j in order[::-1]:
                    if j != which:
                        at_once[j].start()
                outgoing[0] = whole[g * per_unit // LANES]
            elif kind in ("answer", "soon"):
                def answer():
                    few = widened(means(best[other[which]]))
                    if kind == "answer":
                        few = pltpu.roll(few, lax.rem(other[which] * per_unit, LANES), 1)
                    outgoing[which] = few
                    if which:
                        results[which].start()

                if now is True:
                    answer()
                else:
                    pl.when(now)(answer)
                continue
            if now:
                catch_up(have, ready if now is True else now, done)

    last = chunks - 1
    docs_first = [("p", 0, True)] + [("q", j, True) for j in order[:1]]
    for c in range(chunks):
        docs_first += [("y", c, True)] + [("r", c - 1, True)] * (c > 0)
    docs_first.append(("r", last, True))
    docs_first += [("answer", j, True) for j in order[:1]]
    for j in order[2:] + order[1:2]:
        docs_first += [("q", j, True), ("answer", j, True)]
    docs_first += [("share", 0, False)] * short + [("answer", 0, True)]

    def opening(hand):
        return ([("p", 0, True)] + [("q", j, True) for j in order[:1]] + [("give", 0, False)] * hand
                + [("y", 0, True)] + [step for c in range(1, last) for step in (("y", c, False), ("r", c - 1, True))]
                + [("q", j, True) for j in order[1:2]] + [("y", last, False)])

    far = [("q", j, True) for j in order[2:]]
    if short:
        third = opening(False) + far + [("r", last - 1, False), ("r", last, (3,)), ("soon", 3, True), ("rest", 3, False)]
        fourth = opening(True) + [("r", last - 1, (2,)), ("soon", 2, sooner)] + far
        fourth += [("r", last, (2,)), ("soon", 2, jnp.logical_not(sooner)), ("rest", 2, False)]
        plans = [(lax.rem(g, 4) < 2, docs_first), (lax.rem(g, 4) == 2, third), (lax.rem(g, 4) == 3, fourth)]
    else:
        plans = [(True, docs_first)]
    for when, plan in plans:
        if when is True:
            run(plan)
        else:
            pl.when(when)(functools.partial(run, plan))

    if short:
        @pl.when(home)
        def _():
            share.wait_recv()
            for n in range(2):
                for j in range(tail):
                    sim = lax.dot_general(hbuf[n, j], qbuf[g], (((1,), (1,)), ((), ())), preferred_element_type=jnp.float32)
                    rest_best[n * tail + j:n * tail + j + 1, :] = jnp.max(sim, axis=0, keepdims=True)
            extra[...] = widened(means(rest_best[...]))

        @pl.when(jnp.logical_or(home, giver))
        def _():
            give.wait_send()

    def picked(piece, lanes):
        return jnp.take_along_axis(piece, lanes, axis=1, mode="promise_in_bounds")

    sent = [remote(dbuf.at[pl.ds(0, 3)], dbuf.at[pl.ds(0, 3)], d_send, p_recv, partner)]
    if order:
        sent.append(remote(qbuf.at[pl.ds(0, groups - 1)], qbuf.at[pl.ds(0, groups - 1)], q_send, p_recv, partner))
    out = picked(outgoing[0], lane)
    for copy in sent:
        copy.wait_send()
    if order:
        back = remote(pieces.at[pl.ds(0, groups - 1)], pieces.at[pl.ds(0, groups - 1)], o_send, o_recv, partner)
        back.wait_recv()
        for j in order:
            out = jnp.where(source == other[j], picked(pieces[other[j]], lane), out)
        back.wait_send()
    if short:
        row = lax.rem(cand, docs) - late
        mine_whole = (source == top) & jnp.logical_not(same) & (row >= 0) & home
        out = jnp.where(mine_whole, picked(extra[...], jnp.where(mine_whole, row + jnp.where(near, 0, tail), 0)), out)
    out_ref[...] = out


def body(shards, queries, doc_tokens, doc_lens, candidates):
    count, tokens, width = queries.shape
    docs, rows, _ = doc_tokens.shape
    groups = shards // 4
    chunks = len(cut_points(docs)) - 1
    tail = docs - cut_points(docs)[-2]
    q_rows = count * tokens
    blocks = groups * 4 * docs // LANES
    dma = pltpu.SemaphoreType.DMA
    return pl.pallas_call(
        functools.partial(score_kernel, groups, tokens),
        out_shape=pltpu.VMEM(candidates.shape, jnp.float32),
        in_specs=[pl.BlockSpec(memory_space=pl.ANY)] * 4,
        out_specs=pl.BlockSpec(memory_space=pltpu.VMEM),
        scratch_shapes=[
            pltpu.SMEM(doc_lens.shape, jnp.int32),
            pltpu.VMEM(candidates.shape, jnp.int32),
            pltpu.VMEM((groups, q_rows, width), queries.dtype),
            pltpu.VMEM((4, docs, rows, width), doc_tokens.dtype),
            pltpu.VMEM((2, tail, rows, width), doc_tokens.dtype),
            pltpu.VMEM((groups, 4 * docs, q_rows), jnp.float32),
            pltpu.VMEM((2 * tail, q_rows), jnp.float32),
            pltpu.VMEM((groups, count, LANES), jnp.float32),
            pltpu.VMEM((blocks, count, LANES), jnp.float32),
            pltpu.VMEM((groups, count, LANES), jnp.float32),
            pltpu.VMEM((count, LANES), jnp.float32),
            dma((4,)),
            pltpu.SemaphoreType.REGULAR((groups + 1,)),
            dma, dma((groups - 1,)),
            dma, dma, dma((chunks,)), dma((chunks,)),
            dma, dma,
            dma, dma((2,)),
        ],
        compiler_params=pltpu.CompilerParams(collective_id=0, has_side_effects=True),
    )(doc_lens, queries.reshape(q_rows, width), doc_tokens, candidates)


def solution(mesh):
    in_specs = (
        P(("parts", "shard"), None, None),
        P(("parts", "shard"), None, None),
        P(("parts", "shard")),
        P(("parts", "shard"), None),
    )
    out_specs = P(("parts", "shard"), None)
    step = functools.partial(body, mesh.shape["shard"])
    return jax.shard_map(step, mesh=mesh, in_specs=in_specs, out_specs=out_specs, check_vma=False)
```

```python
import functools

import jax
import jax.numpy as jnp
from jax import lax
from jax.experimental import pallas as pl
from jax.experimental.pallas import tpu as pltpu
from jax.sharding import PartitionSpec as P

LANES = 128
MESH = pl.DeviceIdType.MESH


def flip(index, mask):
    out = index
    bit = 1
    while bit <= mask:
        if mask & bit:
            out = out + bit - 2 * bit * ((index // bit) % 2)
        bit *= 2
    return out


def cut_points(docs):
    return [0, 3, 5, 8]


def score_kernel(groups, tokens, lens_hbm, q_hbm, d_hbm, cand_hbm, out_ref,
                 lens_ref, cand_ref, qbuf, dbuf, hbuf, best, rest_best, outgoing, whole, pieces, extra,
                 local_sem, here, q_send, q_recv, d_send, p_recv, y_recv, f_recv, o_send, o_recv, h_send, h_recv):
    part = lax.axis_index("parts")
    me = lax.axis_index("shard")
    k = lax.rem(me, 2)
    b = lax.rem(me // 2, 2)
    g = me // 4

    def at(g_, b_, k_):
        return (part, g_ * 4 + b_ * 2 + k_)

    docs, rows, width = d_hbm.shape
    q_rows = q_hbm.shape[0]
    count = q_rows // tokens
    per_unit = 4 * docs
    edges = cut_points(docs)
    chunks = len(edges) - 1
    order = list(range(1, groups))
    end = lax.rem(g, 4) == 0
    mask = {j: jnp.where(end, j, j ^ 1) if j % 4 > 1 else j for j in order}
    other = {j: jnp.where(end, flip(g, j), flip(g, j ^ 1)) if j % 4 > 1 else flip(g, j) for j in order}
    other[0] = g
    partner = at(g, b, 1 - k)
    across = at(g, 1 - b, 1 - k)
    level = {j: at(other[j], b, 1 - k) for j in order}

    short = groups % 4 == 0
    late = edges[-2]
    tail = docs - late
    home = jnp.logical_and(lax.rem(g, 4) == 0, b == 0)
    sooner = jnp.logical_and(lax.rem(g, 4) == 3, b == 0)
    giver = jnp.logical_and(lax.rem(g, 4) == 3, b == 1)
    top = flip(g, 3)

    def remote(src, dst, send, recv, device):
        return pltpu.make_async_remote_copy(src_ref=src, dst_ref=dst, send_sem=send, recv_sem=recv,
                                            device_id=device, device_id_type=MESH)

    lens_in = pltpu.make_async_copy(lens_hbm, lens_ref, local_sem.at[0])
    q_in = pltpu.make_async_copy(q_hbm, qbuf.at[g], local_sem.at[1])
    cand_in = pltpu.make_async_copy(cand_hbm, cand_ref, local_sem.at[2])
    d_in = pltpu.make_async_copy(d_hbm, dbuf.at[0], local_sem.at[3])
    lens_in.start()
    d_in.start()
    q_in.start()
    cand_in.start()

    pairs = [(0, partner, k == 1), (1, across, b == 0)] + [(1 + mask[j], level[j], g < other[j]) for j in order]
    barrier = pltpu.get_barrier_semaphore()
    greeted = 0
    for _, peer, first in pairs:
        greeted = greeted + jnp.where(first, 0, 1)

        @pl.when(first)
        def _():
            pl.semaphore_signal(barrier, inc=1, device_id=peer, device_id_type=MESH)

    if short:
        greeted = greeted + jnp.where(giver, 1, 0)

        @pl.when(home)
        def _():
            pl.semaphore_signal(barrier, inc=1, device_id=at(top, 1, 1 - k), device_id_type=MESH)

    @pl.when(greeted > 0)
    def _():
        pl.semaphore_wait(barrier, greeted)

    for slot, peer, first in pairs:
        @pl.when(jnp.logical_not(first))
        def _():
            pl.semaphore_signal(here.at[slot], inc=1, device_id=peer, device_id_type=MESH)

    def meet(which):
        slot, _, first = pairs[which]

        @pl.when(first)
        def _():
            pl.semaphore_wait(here.at[slot], 1)

    mine = qbuf.at[g]
    q_out = {j: remote(mine, mine, q_send, q_recv.at[mask[j] - 1], level[j]) for j in order}
    to_partner = remote(dbuf.at[0], dbuf.at[1], d_send, p_recv, partner)
    to_across, relays = [], []
    for c in range(chunks):
        span = pl.ds(edges[c], edges[c + 1] - edges[c])
        to_across.append(remote(dbuf.at[0, span], dbuf.at[2, span], d_send, y_recv.at[c], across))
        relays.append(remote(dbuf.at[2, span], dbuf.at[3, span], d_send, f_recv.at[c], partner))

    lens_in.wait()
    d_in.wait()
    row_of = lax.broadcasted_iota(jnp.int32, (rows, width), 0)
    for c in range(chunks):
        for j in range(edges[c], edges[c + 1]):
            block = dbuf[0, j]
            first_row = jnp.broadcast_to(block[0:1, :].astype(jnp.float32), (rows, width))
            kept = jnp.where(row_of < lens_ref[j], block.astype(jnp.float32), first_row)
            dbuf[0, j] = kept.astype(dbuf.dtype)
        if c == 0:
            meet(1)
        to_across[c].start()
    meet(0)
    to_partner.start()
    q_in.wait()

    def dot_max(unit, which, low, high):
        block = qbuf[other[unit]]
        for j in range(low, high):
            sim = lax.dot_general(dbuf[which, j], block, (((1,), (1,)), ((), ())), preferred_element_type=jnp.float32)
            best[other[unit], which * docs + j:which * docs + j + 1, :] = jnp.max(sim, axis=0, keepdims=True)

    def catch_up(have, units, done):
        for which in range(4):
            for unit in units:
                low = done.get((unit, which), 0)
                if low < have[which]:
                    dot_max(unit, which, low, have[which])
                    done[unit, which] = have[which]

    if order:
        meet(2)
        q_out[order[0]].start()
    dot_max(0, 0, 0, docs)
    swapped = lax.rem(g, 4) == 2
    for j in order[1:]:
        out_mask, out_level = mask[j], other[j]
        if short and j % 4 > 1:
            out_mask = jnp.where(swapped, mask[j ^ 1], out_mask)
            out_level = jnp.where(swapped, other[j ^ 1], out_level)

        @pl.when(g < out_level)
        def _():
            pl.semaphore_wait(here.at[1 + out_mask], 1)

        remote(mine, mine, q_send, q_recv.at[out_mask - 1], at(out_level, b, 1 - k)).start()

    give = remote(dbuf.at[0, pl.ds(late, tail)], hbuf.at[0], h_send, h_recv.at[0], at(top, 0, 1 - k))
    share = remote(hbuf.at[0], hbuf.at[1], h_send, h_recv.at[1], partner)
    cand_in.wait()
    cand = cand_ref[...]
    device = cand // docs
    same = lax.rem(device // 2, 2) == b
    source = device // 4
    holder = jnp.where(source == g, k, 1 - k)
    near = lax.rem(device, 2) == holder
    local = jnp.where(same, jnp.where(near, 0, docs), jnp.where(near, 3 * docs, 2 * docs))
    lane = lax.rem(g * per_unit, LANES) + lax.rem(cand, docs) + local

    q_of = lax.broadcasted_iota(jnp.int32, (count, q_rows), 1) // tokens
    pick = (q_of == lax.broadcasted_iota(jnp.int32, (count, q_rows), 0)).astype(jnp.float32)
    pick = (pick * (1.0 / tokens)).astype(jnp.bfloat16)

    def means(rest):
        total = None
        for _ in range(2):
            term = rest.astype(jnp.bfloat16)
            rest = rest - term.astype(jnp.float32)
            got = lax.dot_general(pick, term, (((1,), (1,)), ((), ())), preferred_element_type=jnp.float32)
            total = got if total is None else total + got
        return total

    def widened(few):
        return jnp.concatenate([few, jnp.zeros((count, LANES - few.shape[1]), jnp.float32)], axis=1)

    blocks = groups * per_unit // LANES
    results = {j: remote(outgoing.at[j], pieces.at[g], o_send, o_recv, level[j]) for j in order}
    at_once = {j: remote(whole.at[other[j] * per_unit // LANES], pieces.at[g], o_send, o_recv, level[j]) for j in order}

    def run(plan):
        have, ready, done = [docs, 0, 0, 0], [0], {(0, 0): docs}
        for kind, which, now in plan:
            if kind == "p":
                to_partner.wait_recv()
                have[1] = docs
            elif kind == "q":
                q_out[which].wait_recv()
                ready.append(which)
            elif kind == "y":
                to_across[which].wait_recv()
                relays[which].start()
                have[2] = edges[which + 1]
            elif kind == "r":
                relays[which].wait_recv()
                have[3] = edges[which + 1]
            elif kind == "give":
                @pl.when(giver)
                def _():
                    give.start()
            elif kind == "share":
                @pl.when(home)
                def _():
                    give.wait_recv()
                    share.start()
            elif kind == "rest":
                catch_up(have, ready, done)
                total = means(best[...].reshape(groups * per_unit, q_rows))
                for n in range(blocks):
                    whole[n] = total[:, n * LANES:(n + 1) * LANES]
                for j in order[::-1]:
                    if j != which:
                        at_once[j].start()
                outgoing[0] = whole[g * per_unit // LANES]
            elif kind in ("answer", "soon"):
                def answer():
                    few = widened(means(best[other[which]]))
                    if kind == "answer":
                        few = pltpu.roll(few, lax.rem(other[which] * per_unit, LANES), 1)
                    outgoing[which] = few
                    if which:
                        results[which].start()

                if now is True:
                    answer()
                else:
                    pl.when(now)(answer)
                continue
            if now:
                catch_up(have, ready if now is True else now, done)

    last = chunks - 1
    docs_first = [("p", 0, True)] + [("q", j, True) for j in order[:1]]
    for c in range(chunks):
        docs_first += [("y", c, True)] + [("r", c - 1, True)] * (c > 0)
    docs_first.append(("r", last, True))
    docs_first += [("answer", j, True) for j in order[:1]]
    for j in order[2:] + order[1:2]:
        docs_first += [("q", j, True), ("answer", j, True)]
    docs_first += [("share", 0, False)] * short + [("answer", 0, True)]

    def opening(hand, early=False):
        return ([("p", 0, True)] + [("give", 0, False)] * hand + [("q", j, True) for j in order[:1]]
                + [("y", 0, True)] + [step for c in range(1, last) for step in (("y", c, False), ("r", c - 1, True))]
                + [("y", last, False)] * early + [("q", j, True) for j in order[1:2]] + [("y", last, False)] * (not early))

    far = [("q", j, True) for j in order[2:]]
    if short:
        third = opening(False, True)[:-1] + [("q", 2, False)] + [("q", 3, (3,))] + [("r", last - 1, False), ("r", last, (3,)), ("soon", 3, True), ("rest", 3, False)]
        fourth = opening(True) + [("r", last - 1, (2,)), ("soon", 2, sooner)] + far
        fourth += [("r", last, (2,)), ("soon", 2, jnp.logical_not(sooner)), ("rest", 2, False)]
        plans = [(lax.rem(g, 4) < 2, docs_first), (lax.rem(g, 4) == 2, third), (lax.rem(g, 4) == 3, fourth)]
    else:
        plans = [(True, docs_first)]
    for when, plan in plans:
        if when is True:
            run(plan)
        else:
            pl.when(when)(functools.partial(run, plan))

    if short:
        @pl.when(home)
        def _():
            share.wait_recv()
            for n in range(2):
                for j in range(tail):
                    sim = lax.dot_general(hbuf[n, j], qbuf[g], (((1,), (1,)), ((), ())), preferred_element_type=jnp.float32)
                    rest_best[n * tail + j:n * tail + j + 1, :] = jnp.max(sim, axis=0, keepdims=True)
            extra[...] = widened(means(rest_best[...]))

        @pl.when(jnp.logical_or(home, giver))
        def _():
            give.wait_send()

    def picked(piece, lanes):
        return jnp.take_along_axis(piece, lanes, axis=1, mode="promise_in_bounds")

    sent = [remote(dbuf.at[pl.ds(0, 3)], dbuf.at[pl.ds(0, 3)], d_send, p_recv, partner)]
    if order:
        sent.append(remote(qbuf.at[pl.ds(0, groups - 1)], qbuf.at[pl.ds(0, groups - 1)], q_send, p_recv, partner))
    out = picked(outgoing[0], lane)
    for copy in sent:
        copy.wait_send()
    if order:
        back = remote(pieces.at[pl.ds(0, groups - 1)], pieces.at[pl.ds(0, groups - 1)], o_send, o_recv, partner)
        back.wait_recv()
        for j in order:
            out = jnp.where(source == other[j], picked(pieces[other[j]], lane), out)
        back.wait_send()
    if short:
        row = lax.rem(cand, docs) - late
        mine_whole = (source == top) & jnp.logical_not(same) & (row >= 0) & home
        out = jnp.where(mine_whole, picked(extra[...], jnp.where(mine_whole, row + jnp.where(near, 0, tail), 0)), out)
    out_ref[...] = out


def body(shards, queries, doc_tokens, doc_lens, candidates):
    count, tokens, width = queries.shape
    docs, rows, _ = doc_tokens.shape
    groups = shards // 4
    chunks = len(cut_points(docs)) - 1
    tail = docs - cut_points(docs)[-2]
    q_rows = count * tokens
    blocks = groups * 4 * docs // LANES
    dma = pltpu.SemaphoreType.DMA
    return pl.pallas_call(
        functools.partial(score_kernel, groups, tokens),
        out_shape=pltpu.VMEM(candidates.shape, jnp.float32),
        in_specs=[pl.BlockSpec(memory_space=pl.ANY)] * 4,
        out_specs=pl.BlockSpec(memory_space=pltpu.VMEM),
        scratch_shapes=[
            pltpu.SMEM(doc_lens.shape, jnp.int32),
            pltpu.VMEM(candidates.shape, jnp.int32),
            pltpu.VMEM((groups, q_rows, width), queries.dtype),
            pltpu.VMEM((4, docs, rows, width), doc_tokens.dtype),
            pltpu.VMEM((2, tail, rows, width), doc_tokens.dtype),
            pltpu.VMEM((groups, 4 * docs, q_rows), jnp.float32),
            pltpu.VMEM((2 * tail, q_rows), jnp.float32),
            pltpu.VMEM((groups, count, LANES), jnp.float32),
            pltpu.VMEM((blocks, count, LANES), jnp.float32),
            pltpu.VMEM((groups, count, LANES), jnp.float32),
            pltpu.VMEM((count, LANES), jnp.float32),
            dma((4,)),
            pltpu.SemaphoreType.REGULAR((groups + 1,)),
            dma, dma((groups - 1,)),
            dma, dma, dma((chunks,)), dma((chunks,)),
            dma, dma,
            dma, dma((2,)),
        ],
        compiler_params=pltpu.CompilerParams(collective_id=0, has_side_effects=True),
    )(doc_lens, queries.reshape(q_rows, width), doc_tokens, candidates)


def solution(mesh):
    in_specs = (
        P(("parts", "shard"), None, None),
        P(("parts", "shard"), None, None),
        P(("parts", "shard")),
        P(("parts", "shard"), None),
    )
    out_specs = P(("parts", "shard"), None)
    step = functools.partial(body, mesh.shape["shard"])
    return jax.shard_map(step, mesh=mesh, in_specs=in_specs, out_specs=out_specs, check_vma=False)
```

```python
import functools

import jax
import jax.numpy as jnp
from jax import lax
from jax.experimental import pallas as pl
from jax.experimental.pallas import tpu as pltpu
from jax.sharding import PartitionSpec as P

LANES = 128
MESH = pl.DeviceIdType.MESH


def flip(index, mask):
    out = index
    bit = 1
    while bit <= mask:
        if mask & bit:
            out = out + bit - 2 * bit * ((index // bit) % 2)
        bit *= 2
    return out


def cut_points(docs):
    return [0, 3, 5, 8]


def score_kernel(groups, tokens, lens_hbm, q_hbm, d_hbm, cand_hbm, out_ref,
                 lens_ref, cand_ref, qbuf, dbuf, hbuf, best, rest_best, outgoing, whole, pieces, extra,
                 local_sem, here, q_send, q_recv, d_send, p_recv, y_recv, f_recv, o_send, o_recv, h_send, h_recv):
    part = lax.axis_index("parts")
    me = lax.axis_index("shard")
    k = lax.rem(me, 2)
    b = lax.rem(me // 2, 2)
    g = me // 4

    def at(g_, b_, k_):
        return (part, g_ * 4 + b_ * 2 + k_)

    docs, rows, width = d_hbm.shape
    q_rows = q_hbm.shape[0]
    count = q_rows // tokens
    per_unit = 4 * docs
    edges = cut_points(docs)
    chunks = len(edges) - 1
    order = list(range(1, groups))
    end = lax.rem(g, 4) == 0
    mask = {j: jnp.where(end, j, j ^ 1) if j % 4 > 1 else j for j in order}
    other = {j: jnp.where(end, flip(g, j), flip(g, j ^ 1)) if j % 4 > 1 else flip(g, j) for j in order}
    other[0] = g
    partner = at(g, b, 1 - k)
    across = at(g, 1 - b, 1 - k)
    level = {j: at(other[j], b, 1 - k) for j in order}

    short = groups % 4 == 0
    late = edges[-2]
    tail = docs - late
    home = jnp.logical_and(lax.rem(g, 4) == 0, b == 0)
    sooner = jnp.logical_and(lax.rem(g, 4) == 3, b == 0)
    giver = jnp.logical_and(lax.rem(g, 4) == 3, b == 1)
    top = flip(g, 3)

    def remote(src, dst, send, recv, device):
        return pltpu.make_async_remote_copy(src_ref=src, dst_ref=dst, send_sem=send, recv_sem=recv,
                                            device_id=device, device_id_type=MESH)

    lens_in = pltpu.make_async_copy(lens_hbm, lens_ref, local_sem.at[0])
    q_in = pltpu.make_async_copy(q_hbm, qbuf.at[g], local_sem.at[1])
    cand_in = pltpu.make_async_copy(cand_hbm, cand_ref, local_sem.at[2])
    d_in = pltpu.make_async_copy(d_hbm, dbuf.at[0], local_sem.at[3])
    lens_in.start()
    d_in.start()
    q_in.start()
    cand_in.start()

    pairs = [(0, partner, k == 1), (1, across, b == 0)] + [(1 + mask[j], level[j], g < other[j]) for j in order]
    barrier = pltpu.get_barrier_semaphore()
    greeted = 0
    for _, peer, first in pairs:
        greeted = greeted + jnp.where(first, 0, 1)

        @pl.when(first)
        def _():
            pl.semaphore_signal(barrier, inc=1, device_id=peer, device_id_type=MESH)

    if short:
        greeted = greeted + jnp.where(giver, 1, 0)

        @pl.when(home)
        def _():
            pl.semaphore_signal(barrier, inc=1, device_id=at(top, 1, 1 - k), device_id_type=MESH)

    @pl.when(greeted > 0)
    def _():
        pl.semaphore_wait(barrier, greeted)

    for slot, peer, first in pairs:
        @pl.when(jnp.logical_not(first))
        def _():
            pl.semaphore_signal(here.at[slot], inc=1, device_id=peer, device_id_type=MESH)

    def meet(which):
        slot, _, first = pairs[which]

        @pl.when(first)
        def _():
            pl.semaphore_wait(here.at[slot], 1)

    mine = qbuf.at[g]
    q_out = {j: remote(mine, mine, q_send, q_recv.at[mask[j] - 1], level[j]) for j in order}
    to_partner = remote(dbuf.at[0], dbuf.at[1], d_send, p_recv, partner)
    to_across, relays = [], []
    for c in range(chunks):
        span = pl.ds(edges[c], edges[c + 1] - edges[c])
        to_across.append(remote(dbuf.at[0, span], dbuf.at[2, span], d_send, y_recv.at[c], across))
        relays.append(remote(dbuf.at[2, span], dbuf.at[3, span], d_send, f_recv.at[c], partner))

    lens_in.wait()
    d_in.wait()
    row_of = lax.broadcasted_iota(jnp.int32, (rows, width), 0)
    for c in range(chunks):
        for j in range(edges[c], edges[c + 1]):
            block = dbuf[0, j]
            first_row = jnp.broadcast_to(block[0:1, :].astype(jnp.float32), (rows, width))
            kept = jnp.where(row_of < lens_ref[j], block.astype(jnp.float32), first_row)
            dbuf[0, j] = kept.astype(dbuf.dtype)
        if c == 0:
            meet(1)
        to_across[c].start()
    meet(0)
    to_partner.start()
    q_in.wait()

    def dot_max(unit, which, low, high):
        block = qbuf[other[unit]]
        for j in range(low, high):
            sim = lax.dot_general(dbuf[which, j], block, (((1,), (1,)), ((), ())), preferred_element_type=jnp.float32)
            best[other[unit], which * docs + j:which * docs + j + 1, :] = jnp.max(sim, axis=0, keepdims=True)

    def catch_up(have, units, done):
        for which in range(4):
            for unit in units:
                low = done.get((unit, which), 0)
                if low < have[which]:
                    dot_max(unit, which, low, have[which])
                    done[unit, which] = have[which]

    if order:
        meet(2)
        q_out[order[0]].start()
    dot_max(0, 0, 0, docs)
    swapped = lax.rem(g, 4) == 2
    give = remote(dbuf.at[0, pl.ds(late, tail)], hbuf.at[0], h_send, h_recv.at[0], at(top, 0, 1 - k))
    share = remote(hbuf.at[0], hbuf.at[1], h_send, h_recv.at[1], partner)
    for j in order[1:]:
        if short and j == 3:
            @pl.when(jnp.logical_and(giver, k == 0))
            def _():
                give.start()

        out_mask, out_level = mask[j], other[j]
        if short and j % 4 > 1:
            out_mask = jnp.where(swapped, mask[j ^ 1], out_mask)
            out_level = jnp.where(swapped, other[j ^ 1], out_level)

        @pl.when(g < out_level)
        def _():
            pl.semaphore_wait(here.at[1 + out_mask], 1)

        remote(mine, mine, q_send, q_recv.at[out_mask - 1], at(out_level, b, 1 - k)).start()

    cand_in.wait()
    cand = cand_ref[...]
    device = cand // docs
    same = lax.rem(device // 2, 2) == b
    source = device // 4
    holder = jnp.where(source == g, k, 1 - k)
    near = lax.rem(device, 2) == holder
    local = jnp.where(same, jnp.where(near, 0, docs), jnp.where(near, 3 * docs, 2 * docs))
    lane = lax.rem(g * per_unit, LANES) + lax.rem(cand, docs) + local

    q_of = lax.broadcasted_iota(jnp.int32, (count, q_rows), 1) // tokens
    pick = (q_of == lax.broadcasted_iota(jnp.int32, (count, q_rows), 0)).astype(jnp.float32)
    pick = (pick * (1.0 / tokens)).astype(jnp.bfloat16)

    def means(rest):
        total = None
        for _ in range(2):
            term = rest.astype(jnp.bfloat16)
            rest = rest - term.astype(jnp.float32)
            got = lax.dot_general(pick, term, (((1,), (1,)), ((), ())), preferred_element_type=jnp.float32)
            total = got if total is None else total + got
        return total

    def widened(few):
        return jnp.concatenate([few, jnp.zeros((count, LANES - few.shape[1]), jnp.float32)], axis=1)

    blocks = groups * per_unit // LANES
    results = {j: remote(outgoing.at[j], pieces.at[g], o_send, o_recv, level[j]) for j in order}
    at_once = {j: remote(whole.at[other[j] * per_unit // LANES], pieces.at[g], o_send, o_recv, level[j]) for j in order}

    def run(plan):
        have, ready, done = [docs, 0, 0, 0], [0], {(0, 0): docs}
        for kind, which, now in plan:
            if kind == "p":
                to_partner.wait_recv()
                have[1] = docs
            elif kind == "q":
                q_out[which].wait_recv()
                ready.append(which)
            elif kind == "y":
                to_across[which].wait_recv()
                relays[which].start()
                have[2] = edges[which + 1]
            elif kind == "r":
                relays[which].wait_recv()
                have[3] = edges[which + 1]
            elif kind == "give":
                @pl.when(jnp.logical_and(giver, k == 1))
                def _():
                    give.start()
            elif kind == "share":
                @pl.when(home)
                def _():
                    give.wait_recv()
                    share.start()
            elif kind == "rest":
                catch_up(have, ready, done)
                total = means(best[...].reshape(groups * per_unit, q_rows))
                for n in range(blocks):
                    whole[n] = total[:, n * LANES:(n + 1) * LANES]
                for j in order[::-1]:
                    if j != which:
                        at_once[j].start()
                outgoing[0] = whole[g * per_unit // LANES]
            elif kind in ("answer", "soon"):
                def answer():
                    few = widened(means(best[other[which]]))
                    if kind == "answer":
                        few = pltpu.roll(few, lax.rem(other[which] * per_unit, LANES), 1)
                    outgoing[which] = few
                    if which:
                        results[which].start()

                if now is True:
                    answer()
                else:
                    pl.when(now)(answer)
                continue
            if now:
                catch_up(have, ready if now is True else now, done)

    last = chunks - 1
    docs_first = [("p", 0, True)] + [("q", j, True) for j in order[:1]]
    for c in range(chunks):
        docs_first += [("y", c, True)] + [("r", c - 1, True)] * (c > 0)
    docs_first.append(("r", last, True))
    docs_first += [("answer", j, True) for j in order[:1]]
    for j in order[2:] + order[1:2]:
        docs_first += [("q", j, True), ("answer", j, True)]
    docs_first += [("share", 0, False)] * short + [("answer", 0, True)]

    def opening(hand, early=False):
        return ([("p", 0, True)] + [("give", 0, False)] * hand + [("q", j, True) for j in order[:1]]
                + [("y", 0, True)] + [step for c in range(1, last) for step in (("y", c, False), ("r", c - 1, True))]
                + [("y", last, False)] * early + [("q", j, True) for j in order[1:2]] + [("y", last, False)] * (not early))

    far = [("q", j, True) for j in order[2:]]
    if short:
        third = opening(False, True)[:-1] + [("q", 2, False)] + [("q", 3, (3,))] + [("r", last - 1, False), ("r", last, (3,)), ("soon", 3, True), ("rest", 3, False)]
        fourth = opening(True) + [("r", last - 1, False)] + far
        fourth += [("r", last, (2,)), ("soon", 2, True), ("rest", 2, False)]
        soonest = opening(False)[:-2] + [("q", 2, (2,)), ("r", last - 1, (2,)), ("soon", 2, True), ("y", last, False)] + far
        soonest += [("r", last, False), ("rest", 2, False)]
        plans = [(lax.rem(g, 4) < 2, docs_first), (lax.rem(g, 4) == 2, third), (giver, fourth), (sooner, soonest)]
    else:
        plans = [(True, docs_first)]
    for when, plan in plans:
        if when is True:
            run(plan)
        else:
            pl.when(when)(functools.partial(run, plan))

    if short:
        @pl.when(home)
        def _():
            for n in range(2):
                if n:
                    share.wait_recv()
                for j in range(tail):
                    sim = lax.dot_general(hbuf[n, j], qbuf[g], (((1,), (1,)), ((), ())), preferred_element_type=jnp.float32)
                    rest_best[n * tail + j:n * tail + j + 1, :] = jnp.max(sim, axis=0, keepdims=True)
            extra[...] = widened(means(rest_best[...]))

        @pl.when(jnp.logical_or(home, giver))
        def _():
            give.wait_send()

    def picked(piece, lanes):
        return jnp.take_along_axis(piece, lanes, axis=1, mode="promise_in_bounds")

    sent = [remote(dbuf.at[pl.ds(0, 3)], dbuf.at[pl.ds(0, 3)], d_send, p_recv, partner)]
    if order:
        sent.append(remote(qbuf.at[pl.ds(0, groups - 1)], qbuf.at[pl.ds(0, groups - 1)], q_send, p_recv, partner))
    out = picked(outgoing[0], lane)
    for copy in sent:
        copy.wait_send()
    if short:
        row = lax.rem(cand, docs) - late
        mine_whole = (source == top) & jnp.logical_not(same) & (row >= 0) & home
        given = picked(extra[...], jnp.where(mine_whole, row + jnp.where(near, 0, tail), 0))
    if order:
        back = remote(pieces.at[pl.ds(0, groups - 1)], pieces.at[pl.ds(0, groups - 1)], o_send, o_recv, partner)
        back.wait_recv()
        for j in order:
            out = jnp.where(source == other[j], picked(pieces[other[j]], lane), out)
        back.wait_send()
    if short:
        out = jnp.where(mine_whole, given, out)
    out_ref[...] = out


def body(shards, queries, doc_tokens, doc_lens, candidates):
    count, tokens, width = queries.shape
    docs, rows, _ = doc_tokens.shape
    groups = shards // 4
    chunks = len(cut_points(docs)) - 1
    tail = docs - cut_points(docs)[-2]
    q_rows = count * tokens
    blocks = groups * 4 * docs // LANES
    dma = pltpu.SemaphoreType.DMA
    return pl.pallas_call(
        functools.partial(score_kernel, groups, tokens),
        out_shape=pltpu.VMEM(candidates.shape, jnp.float32),
        in_specs=[pl.BlockSpec(memory_space=pl.ANY)] * 4,
        out_specs=pl.BlockSpec(memory_space=pltpu.VMEM),
        scratch_shapes=[
            pltpu.SMEM(doc_lens.shape, jnp.int32),
            pltpu.VMEM(candidates.shape, jnp.int32),
            pltpu.VMEM((groups, q_rows, width), queries.dtype),
            pltpu.VMEM((4, docs, rows, width), doc_tokens.dtype),
            pltpu.VMEM((2, tail, rows, width), doc_tokens.dtype),
            pltpu.VMEM((groups, 4 * docs, q_rows), jnp.float32),
            pltpu.VMEM((2 * tail, q_rows), jnp.float32),
            pltpu.VMEM((groups, count, LANES), jnp.float32),
            pltpu.VMEM((blocks, count, LANES), jnp.float32),
            pltpu.VMEM((groups, count, LANES), jnp.float32),
            pltpu.VMEM((count, LANES), jnp.float32),
            dma((4,)),
            pltpu.SemaphoreType.REGULAR((groups + 1,)),
            dma, dma((groups - 1,)),
            dma, dma, dma((chunks,)), dma((chunks,)),
            dma, dma,
            dma, dma((2,)),
        ],
        compiler_params=pltpu.CompilerParams(collective_id=0, has_side_effects=True),
    )(doc_lens, queries.reshape(q_rows, width), doc_tokens, candidates)


def solution(mesh):
    in_specs = (
        P(("parts", "shard"), None, None),
        P(("parts", "shard"), None, None),
        P(("parts", "shard")),
        P(("parts", "shard"), None),
    )
    out_specs = P(("parts", "shard"), None)
    step = functools.partial(body, mesh.shape["shard"])
    return jax.shard_map(step, mesh=mesh, in_specs=in_specs, out_specs=out_specs, check_vma=False)
```

```python
import functools

import jax
import jax.numpy as jnp
from jax import lax
from jax.experimental import pallas as pl
from jax.experimental.pallas import tpu as pltpu
from jax.sharding import PartitionSpec as P

LANES = 128
MESH = pl.DeviceIdType.MESH


def flip(index, mask):
    out = index
    bit = 1
    while bit <= mask:
        if mask & bit:
            out = out + bit - 2 * bit * ((index // bit) % 2)
        bit *= 2
    return out


def cut_points(docs):
    return [0, docs * 3 // 8, docs * 5 // 8, docs]


def score_kernel(groups, tokens, lens_hbm, q_hbm, d_hbm, cand_hbm, out_ref,
                 lens_ref, cand_ref, qbuf, dbuf, hbuf, best, rest_best, outgoing, whole, pieces, extra,
                 local_sem, here, q_send, q_recv, d_send, p_recv, y_recv, f_recv, o_send, o_recv, h_send, h_recv):
    part = lax.axis_index("parts")
    me = lax.axis_index("shard")
    k = lax.rem(me, 2)
    b = lax.rem(me // 2, 2)
    g = me // 4

    def at(g_, b_, k_):
        return (part, g_ * 4 + b_ * 2 + k_)

    docs, rows, width = d_hbm.shape
    q_rows = q_hbm.shape[0]
    count = q_rows // tokens
    per_unit = 4 * docs
    edges = cut_points(docs)
    chunks = len(edges) - 1
    order = list(range(1, groups))
    end = lax.rem(g, 4) == 0
    mask = {j: jnp.where(end, j, j ^ 1) if j % 4 > 1 else j for j in order}
    other = {j: jnp.where(end, flip(g, j), flip(g, j ^ 1)) if j % 4 > 1 else flip(g, j) for j in order}
    other[0] = g
    partner = at(g, b, 1 - k)
    across = at(g, 1 - b, 1 - k)
    level = {j: at(other[j], b, 1 - k) for j in order}

    short = groups % 4 == 0
    late = edges[-2]
    tail = docs - late
    home = jnp.logical_and(lax.rem(g, 4) == 0, b == 0)
    sooner = jnp.logical_and(lax.rem(g, 4) == 3, b == 0)
    giver = jnp.logical_and(lax.rem(g, 4) == 3, b == 1)
    top = flip(g, 3)

    def remote(src, dst, send, recv, device):
        return pltpu.make_async_remote_copy(src_ref=src, dst_ref=dst, send_sem=send, recv_sem=recv,
                                            device_id=device, device_id_type=MESH)

    lens_in = pltpu.make_async_copy(lens_hbm, lens_ref, local_sem.at[0])
    q_in = pltpu.make_async_copy(q_hbm, qbuf.at[g], local_sem.at[1])
    cand_in = pltpu.make_async_copy(cand_hbm, cand_ref, local_sem.at[2])
    d_in = pltpu.make_async_copy(d_hbm, dbuf.at[0], local_sem.at[3])
    lens_in.start()
    d_in.start()
    q_in.start()
    cand_in.start()

    pairs = [(0, partner, k == 1), (1, across, b == 0)] + [(1 + mask[j], level[j], g < other[j]) for j in order]
    barrier = pltpu.get_barrier_semaphore()
    greeted = 0
    for _, peer, first in pairs:
        greeted = greeted + jnp.where(first, 0, 1)

        @pl.when(first)
        def _():
            pl.semaphore_signal(barrier, inc=1, device_id=peer, device_id_type=MESH)

    if short:
        greeted = greeted + jnp.where(giver, 1, 0)

        @pl.when(home)
        def _():
            pl.semaphore_signal(barrier, inc=1, device_id=at(top, 1, 1 - k), device_id_type=MESH)

    @pl.when(greeted > 0)
    def _():
        pl.semaphore_wait(barrier, greeted)

    for slot, peer, first in pairs:
        @pl.when(jnp.logical_not(first))
        def _():
            pl.semaphore_signal(here.at[slot], inc=1, device_id=peer, device_id_type=MESH)

    def meet(which):
        slot, _, first = pairs[which]

        @pl.when(first)
        def _():
            pl.semaphore_wait(here.at[slot], 1)

    mine = qbuf.at[g]
    q_out = {j: remote(mine, mine, q_send, q_recv.at[mask[j] - 1], level[j]) for j in order}
    to_partner = remote(dbuf.at[0], dbuf.at[1], d_send, p_recv, partner)
    to_across, relays = [], []
    for c in range(chunks):
        span = pl.ds(edges[c], edges[c + 1] - edges[c])
        to_across.append(remote(dbuf.at[0, span], dbuf.at[2, span], d_send, y_recv.at[c], across))
        relays.append(remote(dbuf.at[2, span], dbuf.at[3, span], d_send, f_recv.at[c], partner))

    lens_in.wait()
    d_in.wait()
    row_of = lax.broadcasted_iota(jnp.int32, (rows, width), 0)
    for c in range(chunks):
        for j in range(edges[c], edges[c + 1]):
            block = dbuf[0, j]
            first_row = jnp.broadcast_to(block[0:1, :].astype(jnp.float32), (rows, width))
            kept = jnp.where(row_of < lens_ref[j], block.astype(jnp.float32), first_row)
            dbuf[0, j] = kept.astype(dbuf.dtype)
        if c == 0:
            meet(1)
        to_across[c].start()
    meet(0)
    to_partner.start()
    q_in.wait()

    def dot_max(unit, which, low, high):
        block = qbuf[other[unit]]
        for j in range(low, high):
            sim = lax.dot_general(dbuf[which, j], block, (((1,), (1,)), ((), ())), preferred_element_type=jnp.float32)
            best[other[unit], which * docs + j:which * docs + j + 1, :] = jnp.max(sim, axis=0, keepdims=True)

    def catch_up(have, units, done):
        for which in range(4):
            for unit in units:
                low = done.get((unit, which), 0)
                if low < have[which]:
                    dot_max(unit, which, low, have[which])
                    done[unit, which] = have[which]

    if order:
        meet(2)
        q_out[order[0]].start()
    dot_max(0, 0, 0, docs)
    swapped = lax.rem(g, 4) == 2
    give = remote(dbuf.at[0, pl.ds(late, tail)], hbuf.at[0], h_send, h_recv.at[0], at(top, 0, 1 - k))
    share = remote(hbuf.at[0], hbuf.at[1], h_send, h_recv.at[1], partner)
    for j in order[1:]:
        if short and j == 3:
            @pl.when(jnp.logical_and(giver, k == 0))
            def _():
                give.start()

        out_mask, out_level = mask[j], other[j]
        if short and j % 4 > 1:
            out_mask = jnp.where(swapped, mask[j ^ 1], out_mask)
            out_level = jnp.where(swapped, other[j ^ 1], out_level)

        @pl.when(g < out_level)
        def _():
            pl.semaphore_wait(here.at[1 + out_mask], 1)

        remote(mine, mine, q_send, q_recv.at[out_mask - 1], at(out_level, b, 1 - k)).start()

    cand_in.wait()
    cand = cand_ref[...]
    device = cand // docs
    same = lax.rem(device // 2, 2) == b
    source = device // 4
    holder = jnp.where(source == g, k, 1 - k)
    near = lax.rem(device, 2) == holder
    local = jnp.where(same, jnp.where(near, 0, docs), jnp.where(near, 3 * docs, 2 * docs))
    lane = lax.rem(g * per_unit, LANES) + lax.rem(cand, docs) + local

    q_of = lax.broadcasted_iota(jnp.int32, (count, q_rows), 1) // tokens
    pick = (q_of == lax.broadcasted_iota(jnp.int32, (count, q_rows), 0)).astype(jnp.float32)
    pick = (pick * (1.0 / tokens)).astype(jnp.bfloat16)

    def means(rest):
        total = None
        for _ in range(2):
            term = rest.astype(jnp.bfloat16)
            rest = rest - term.astype(jnp.float32)
            got = lax.dot_general(pick, term, (((1,), (1,)), ((), ())), preferred_element_type=jnp.float32)
            total = got if total is None else total + got
        return total

    def widened(few):
        return jnp.concatenate([few, jnp.zeros((count, LANES - few.shape[1]), jnp.float32)], axis=1)

    blocks = groups * per_unit // LANES
    results = {j: remote(outgoing.at[j], pieces.at[g], o_send, o_recv, level[j]) for j in order}
    at_once = {j: remote(whole.at[other[j] * per_unit // LANES], pieces.at[g], o_send, o_recv, level[j]) for j in order}

    def run(plan):
        have, ready, done = [docs, 0, 0, 0], [0], {(0, 0): docs}
        for kind, which, now in plan:
            if kind == "p":
                to_partner.wait_recv()
                have[1] = docs
            elif kind == "q":
                q_out[which].wait_recv()
                ready.append(which)
            elif kind == "y":
                to_across[which].wait_recv()
                relays[which].start()
                have[2] = edges[which + 1]
            elif kind == "r":
                relays[which].wait_recv()
                have[3] = edges[which + 1]
            elif kind == "give":
                @pl.when(jnp.logical_and(giver, k == 1))
                def _():
                    give.start()
            elif kind == "share":
                @pl.when(home)
                def _():
                    give.wait_recv()
                    share.start()
            elif kind == "rest":
                catch_up(have, ready, done)
                total = means(best[...].reshape(groups * per_unit, q_rows))
                for n in range(blocks):
                    whole[n] = total[:, n * LANES:(n + 1) * LANES]
                for j in order[::-1]:
                    if j != which:
                        at_once[j].start()
                outgoing[0] = whole[g * per_unit // LANES]
            elif kind in ("answer", "soon"):
                def answer():
                    few = widened(means(best[other[which]]))
                    if kind == "answer":
                        few = pltpu.roll(few, lax.rem(other[which] * per_unit, LANES), 1)
                    outgoing[which] = few
                    if which:
                        results[which].start()

                if now is True:
                    answer()
                else:
                    pl.when(now)(answer)
                continue
            if now:
                catch_up(have, ready if now is True else now, done)

    last = chunks - 1
    docs_first = [("p", 0, True)] + [("q", j, True) for j in order[:1]]
    for c in range(chunks):
        docs_first += [("y", c, True)] + [("r", c - 1, True)] * (c > 0)
    docs_first.append(("r", last, True))
    docs_first += [("answer", j, True) for j in order[:1]]
    for j in order[2:] + order[1:2]:
        docs_first += [("q", j, True), ("answer", j, True)]
    docs_first += [("share", 0, False)] * short + [("answer", 0, True)]

    def opening(hand, early=False):
        return ([("p", 0, True)] + [("give", 0, False)] * hand + [("q", j, True) for j in order[:1]]
                + [("y", 0, True)] + [step for c in range(1, last) for step in (("y", c, False), ("r", c - 1, True))]
                + [("y", last, False)] * early + [("q", j, True) for j in order[1:2]] + [("y", last, False)] * (not early))

    far = [("q", j, True) for j in order[2:]]
    if short:
        third = opening(False, True)[:-1] + [("q", 2, False)] + [("q", 3, (3,))] + [("r", last - 1, False), ("r", last, (3,)), ("soon", 3, True)]
        third += [("q", j, False) for j in order[3:]] + [("rest", 3, False)]
        fourth = opening(True) + [("r", last - 1, False)] + far
        fourth += [("r", last, (2,)), ("soon", 2, True), ("rest", 2, False)]
        soonest = opening(False)[:-2] + [("q", 2, (2,)), ("r", last - 1, (2,)), ("soon", 2, True), ("y", last, False)] + far
        soonest += [("r", last, False), ("rest", 2, False)]
        plans = [(lax.rem(g, 4) < 2, docs_first), (lax.rem(g, 4) == 2, third), (giver, fourth), (sooner, soonest)]
    else:
        plans = [(True, docs_first)]
    for when, plan in plans:
        if when is True:
            run(plan)
        else:
            pl.when(when)(functools.partial(run, plan))

    if short:
        @pl.when(home)
        def _():
            for n in range(2):
                if n:
                    share.wait_recv()
                for j in range(tail):
                    sim = lax.dot_general(hbuf[n, j], qbuf[g], (((1,), (1,)), ((), ())), preferred_element_type=jnp.float32)
                    rest_best[n * tail + j:n * tail + j + 1, :] = jnp.max(sim, axis=0, keepdims=True)
            extra[...] = widened(means(rest_best[...]))

        @pl.when(jnp.logical_or(home, giver))
        def _():
            give.wait_send()

    def picked(piece, lanes):
        return jnp.take_along_axis(piece, lanes, axis=1, mode="promise_in_bounds")

    sent = [remote(dbuf.at[pl.ds(0, 3)], dbuf.at[pl.ds(0, 3)], d_send, p_recv, partner)]
    if order:
        sent.append(remote(qbuf.at[pl.ds(0, groups - 1)], qbuf.at[pl.ds(0, groups - 1)], q_send, p_recv, partner))
    out = picked(outgoing[0], lane)
    for copy in sent:
        copy.wait_send()
    if short:
        row = lax.rem(cand, docs) - late
        mine_whole = (source == top) & jnp.logical_not(same) & (row >= 0) & home
        given = picked(extra[...], jnp.where(mine_whole, row + jnp.where(near, 0, tail), 0))
    if order:
        back = remote(pieces.at[pl.ds(0, groups - 1)], pieces.at[pl.ds(0, groups - 1)], o_send, o_recv, partner)
        back.wait_recv()
        for j in order:
            out = jnp.where(source == other[j], picked(pieces[other[j]], lane), out)
        back.wait_send()
    if short:
        out = jnp.where(mine_whole, given, out)
    out_ref[...] = out


def body(shards, queries, doc_tokens, doc_lens, candidates):
    count, tokens, width = queries.shape
    docs, rows, _ = doc_tokens.shape
    groups = shards // 4
    chunks = len(cut_points(docs)) - 1
    tail = docs - cut_points(docs)[-2]
    q_rows = count * tokens
    blocks = groups * 4 * docs // LANES
    dma = pltpu.SemaphoreType.DMA
    return pl.pallas_call(
        functools.partial(score_kernel, groups, tokens),
        out_shape=pltpu.VMEM(candidates.shape, jnp.float32),
        in_specs=[pl.BlockSpec(memory_space=pl.ANY)] * 4,
        out_specs=pl.BlockSpec(memory_space=pltpu.VMEM),
        scratch_shapes=[
            pltpu.SMEM(doc_lens.shape, jnp.int32),
            pltpu.VMEM(candidates.shape, jnp.int32),
            pltpu.VMEM((groups, q_rows, width), queries.dtype),
            pltpu.VMEM((4, docs, rows, width), doc_tokens.dtype),
            pltpu.VMEM((2, tail, rows, width), doc_tokens.dtype),
            pltpu.VMEM((groups, 4 * docs, q_rows), jnp.float32),
            pltpu.VMEM((2 * tail, q_rows), jnp.float32),
            pltpu.VMEM((groups, count, LANES), jnp.float32),
            pltpu.VMEM((blocks, count, LANES), jnp.float32),
            pltpu.VMEM((groups, count, LANES), jnp.float32),
            pltpu.VMEM((count, LANES), jnp.float32),
            dma((4,)),
            pltpu.SemaphoreType.REGULAR((groups + 1,)),
            dma, dma((groups - 1,)),
            dma, dma, dma((chunks,)), dma((chunks,)),
            dma, dma,
            dma, dma((2,)),
        ],
        compiler_params=pltpu.CompilerParams(collective_id=0, has_side_effects=True),
    )(doc_lens, queries.reshape(q_rows, width), doc_tokens, candidates)


def solution(mesh):
    in_specs = (
        P(("parts", "shard"), None, None),
        P(("parts", "shard"), None, None),
        P(("parts", "shard")),
        P(("parts", "shard"), None),
    )
    out_specs = P(("parts", "shard"), None)
    step = functools.partial(body, mesh.shape["shard"])
    return jax.shard_map(step, mesh=mesh, in_specs=in_specs, out_specs=out_specs, check_vma=False)
```
